256 devices in a mesh: row: 8 (over y, core), col: 32 (over x, z).
Axes of the slice: x: 4, y: 4, z: 8, core: 2. Of those that a mesh axis runs over, the one named last changes fastest.
Arguments:
- images: float32 [4, 256, 65536], P(None, 'row', 'col'), may hold values from -6 to 6
Outputs:
- coefficients: float32 [4, 256, 65536], P(None, 'row', 'col')
The draws below stay inside these ranges and needn't reach their ends.
All inputs are finite; a program needn't handle non-finite values.
Results may differ from the reference program's by a relative error of at most 0.00002.
Values sent between devices are 32-bit elements; how exact they have to be, the bound alone decides.
No kernel may reach another device: no remote copies, remote signals or barrier semaphores. Data moves between devices by JAX's collectives and lax.ppermute only.
A program may use at most 128 MiB of HBM per device.

```python
import jax
import jax.numpy as jnp
from jax import lax

IMAGES = 4
LEVELS = 3
NR = 256
NC = 65536


def steps_of(key, extent, cuts, low, high):
    def one(dim, parts):
        steps = jax.random.uniform(jax.random.fold_in(jax.random.fold_in(key, 6), dim), (parts,), jnp.float32, low / len(cuts), high / len(cuts))
        return jnp.repeat(jnp.exp(steps), extent[dim] // parts).reshape((-1,) + (1,) * (len(extent) - dim - 1))

    loudness = one(*cuts[0])
    for cut in cuts[1:]:
        loudness = loudness * one(*cut)
    return loudness


def normal_values(stream_key, dims, scale, most, shards=(), kind=jnp.bfloat16):
    values = scale * jax.random.normal(stream_key, dims, jnp.float32)
    if shards:
        values = values * steps_of(stream_key, dims, shards, -0.22, 0.18)
    return jnp.clip(values, -most, most).astype(kind)


def setup_inputs(seed: int = 0) -> dict:
    key_list = jax.random.split(jax.random.key(seed), 2)
    images = normal_values(key_list[0], (IMAGES, NR, NC), 1.0, 6.0, ((1, 8), (2, 32)), jnp.float32)
    return dict(images=images)


PREDICT_ONE = -1.586134342
UPDATE_ONE = -0.05298011854
PREDICT_TWO = 0.8829110762
UPDATE_TWO = 0.4435068522
SCALE_HIGH = 1.230174105
SCALE_LOW = 1.0 / 1.230174105


def segment(values, start, stop, along):
    return lax.slice_in_dim(values, start, stop, 1, along)


def lifting(extended, along):
    length = extended.shape[along]
    halves = length // 2
    evens = lax.slice_in_dim(extended, 0, length, 2, along)
    odds = lax.slice_in_dim(extended, 1, length, 2, along)
    predicted = segment(odds, 0, halves - 1, along) + PREDICT_ONE * (segment(evens, 0, halves - 1, along) + segment(evens, 1, halves, along))
    updated = segment(evens, 1, halves - 1, along) + UPDATE_ONE * (segment(predicted, 0, halves - 2, along) + segment(predicted, 1, halves - 1, along))
    refined = segment(predicted, 1, halves - 2, along) + PREDICT_TWO * (segment(updated, 0, halves - 3, along) + segment(updated, 1, halves - 2, along))
    smoothed = segment(updated, 1, halves - 3, along) + UPDATE_TWO * (segment(refined, 0, halves - 4, along) + segment(refined, 1, halves - 3, along))
    lowpass = smoothed * SCALE_LOW
    highpass = segment(refined, 1, halves - 3, along) * SCALE_HIGH
    paired = jnp.stack([lowpass, highpass], axis=along + 1)
    shape = list(extended.shape)
    shape[along] = length - 8
    return paired.reshape(shape)


def one_level(lowband):
    extended = jnp.pad(lowband, ((0, 0), (4, 4), (0, 0)), mode="reflect")
    vertical = lifting(extended, 1)
    extended = jnp.pad(vertical, ((0, 0), (0, 0), (4, 4)), mode="reflect")
    return lifting(extended, 2)


def one_image(single):
    lowband = single[None]
    results = []
    for level_index in range(LEVELS):
        transformed = one_level(lowband)
        results.append(transformed)
        lowband = transformed[:, ::2, ::2]
    combined = results[-1]
    for transformed in reversed(results[:-1]):
        combined = transformed.at[:, ::2, ::2].set(combined)
    return combined[0]


def reference(images):
    return lax.map(one_image, images)
```

```python
import jax
import jax.numpy as jnp
from jax import lax
from jax.experimental import pallas as pl
from jax.experimental.pallas import tpu as pltpu
from jax.sharding import PartitionSpec as P

ALPHA = -1.586134342
BETA = -0.05298011854
GAMMA = 0.8829110762
DELTA = 0.4435068522
SCALE_HIGH = 1.230174105
SCALE_LOW = 1.0 / 1.230174105

IMAGES = 4
ROWS = 32
CHUNKS = 16
TILES = IMAGES * CHUNKS
LANES = 128
KINDS = ((0, 4, 8), (4, 2, 16), (6, 1, 32))


def _lift(x, left, right):
    s, d = x[0::2], x[1::2]
    m = len(s)
    d = [d[i] + ALPHA * (s[i] + (s[i + 1] if i + 1 < m else right[0])) for i in range(m)]
    s = [s[i] + BETA * ((d[i - 1] if i else left[0]) + d[i]) for i in range(m)]
    d = [d[i] + GAMMA * (s[i] + (s[i + 1] if i + 1 < m else right[1])) for i in range(m)]
    s = [s[i] + DELTA * ((d[i - 1] if i else left[1]) + d[i]) for i in range(m)]
    return [v * SCALE_LOW for v in s]


def _states(x):
    p = x[-1] + ALPHA * x[-2]
    t = x[-2] + BETA * (x[-3] + ALPHA * (x[-4] + x[-2]))
    s = x[0]
    u = x[0] + BETA * (x[1] + ALPHA * (x[0] + x[2]))
    return p, t, s, u


def _responses():
    zero = (0.0, 0.0)
    end, start = {}, {}
    for level in (1, 2):
        for j in range(2):
            unit = (1.0, 0.0) if j == 0 else (0.0, 1.0)
            for table, left, right, pick in ((end, zero, unit, 0), (start, unit, zero, 2)):
                band = [0.0] * (ROWS >> (level - 1))
                low = _lift(band, left, right)
                for into in range(level + 1, 4):
                    table[level, into, j] = _states(low)[pick : pick + 2]
                    low = _lift(low, zero, zero)
    return end, start


END, START = _responses()


def _rows_of(ref, t):
    return [ref[t, pl.ds(q, 8, stride=4), :] for q in (0, 2, 1, 3)]


def _load_x(x_ref, scr, sems):
    copies = []
    for img in range(IMAGES):
        for rt in range(4):
            copies.append(
                pltpu.make_async_copy(
                    x_ref.at[img, rt],
                    scr.at[pl.ds(img * CHUNKS, CHUNKS), pl.ds(rt * 8, 8), :],
                    sems.at[img, rt],
                )
            )
    for c in copies:
        c.start()
    return copies


def _sub_iota():
    return lax.broadcasted_iota(jnp.int32, (8, LANES), 0)


def states_kernel(x_ref, down_ref, up_ref, scr, sems):
    copies = _load_x(x_ref, scr, sems)
    sub = _sub_iota()
    is7 = sub == 7
    is0 = sub == 0
    odd = (sub & 1) == 1
    zero = jnp.zeros((8, LANES), jnp.float32)

    def up(v):
        return jnp.where(is7, zero, pltpu.roll(v, 7, 0))

    def dn(v):
        return jnp.where(is0, zero, pltpu.roll(v, 1, 0))

    def body(t, carry):
        a, b, c, d = _rows_of(scr, t)
        lo, hi = [], []
        lo.append((d + ALPHA * b)[7:8])
        c1 = c + ALPHA * (a + b)
        lo.append((b + BETA * c1)[7:8])
        hi.append(a[0:1])
        hi.append((a + BETA * c1)[0:1])
        d1 = d + ALPHA * (b + up(a))
        a1 = a + BETA * (dn(d1) + c1)
        b1 = b + BETA * (c1 + d1)
        c2 = c1 + GAMMA * (a1 + b1)
        d2 = d1 + GAMMA * (b1 + up(a1))
        a = (a1 + DELTA * (dn(d2) + c2)) * SCALE_LOW
        b = (b1 + DELTA * (c2 + d2)) * SCALE_LOW
        lo.append((b + ALPHA * a)[7:8])
        b1 = b + ALPHA * (a + up(a))
        rb = dn(b1)
        lo.append((a + BETA * rb)[7:8])
        hi.append(a[0:1])
        hi.append((a + BETA * b1)[0:1])
        a1 = a + BETA * (rb + b1)
        b2 = b1 + GAMMA * (a1 + up(a1))
        x = (a1 + DELTA * (dn(b2) + b2)) * SCALE_LOW
        ru = pltpu.roll(x, 1, 0)
        lo.append((x + ALPHA * ru)[7:8])
        x1 = x + ALPHA * (ru + pltpu.roll(x, 7, 0))
        lo.append((x + BETA * pltpu.roll(x1, 1, 0))[6:7])
        hi.append(x[0:1])
        hi.append((x + BETA * pltpu.roll(x1, 7, 0))[0:1])
        for k in range(6):
            down_ref[pl.ds(k * TILES + t, 1), :] = lo[k]
            up_ref[pl.ds(k * TILES + t, 1), :] = hi[k]
        return carry

    for img in range(IMAGES):
        for rt in range(4):
            copies[img * 4 + rt].wait()
        lax.fori_loop(img * CHUNKS, (img + 1) * CHUNKS, body, 0)


def _boundary(k, ref):
    return ref[pl.ds(k * TILES, TILES), :]


def _junction(ends, starts):
    out = []
    for level in (1, 2, 3):
        p, t = ends[2 * level - 2], ends[2 * level - 1]
        s, u = starts[2 * level - 2], starts[2 * level - 1]
        for prior in range(1, level):
            l1, l2, r1, r2 = out[prior - 1]
            e0, e1 = END[prior, level, 0], END[prior, level, 1]
            s0, s1 = START[prior, level, 0], START[prior, level, 1]
            p = p + e0[0] * r1 + e1[0] * r2
            t = t + e0[1] * r1 + e1[1] * r2
            s = s + s0[0] * l1 + s1[0] * l2
            u = u + s0[1] * l1 + s1[1] * l2
        l1 = p + ALPHA * s
        r2 = u + BETA * l1
        l2 = l1 + GAMMA * (t + BETA * l1 + r2)
        out.append((l1, l2, s, r2))
    return out


def rows_kernel(x_ref, own_end, own_start, got_end, got_start, v_ref, left_ref, right_ref, scr, bnd, sems):
    copies = _load_x(x_ref, scr, sems)
    row = lax.axis_index("row")
    first = row == 0
    last = row == lax.axis_size("row") - 1
    top = _junction([_boundary(k, got_end) for k in range(6)], [_boundary(k, own_start) for k in range(6)])
    for level in range(3):
        for j in range(2):
            bnd[pl.ds((level * 4 + j) * TILES, TILES), :] = top[level][j]
    low = _junction([_boundary(k, own_end) for k in range(6)], [_boundary(k, got_start) for k in range(6)])
    for level in range(3):
        for j in range(2, 4):
            bnd[pl.ds((level * 4 + j) * TILES, TILES), :] = low[level][j]

    sub = _sub_iota()
    is7 = sub == 7
    is0 = sub == 0
    mir7 = is7 & last
    mir0 = is0 & first
    odd = (sub & 1) == 1
    zero = jnp.zeros((8, LANES), jnp.float32)
    c_alpha = jnp.where(odd, ALPHA, zero)
    c_beta = jnp.where(odd, zero, BETA)
    c_gamma = jnp.where(odd, GAMMA, zero)
    c_delta = jnp.where(odd, zero, DELTA)
    c_scale = jnp.where(odd, SCALE_HIGH, SCALE_LOW).astype(jnp.float32)

    def body(t, carry):
        def edge(level, j):
            return jnp.broadcast_to(bnd[pl.ds(((level - 1) * 4 + j) * TILES + t, 1), :], (8, LANES))

        def up(v, level, j, mirror):
            return jnp.where(mir7, mirror, jnp.where(is7, edge(level, j), pltpu.roll(v, 7, 0)))

        def dn(v, level, j, mirror):
            return jnp.where(mir0, mirror, jnp.where(is0, edge(level, j), pltpu.roll(v, 1, 0)))

        a, b, c, d = _rows_of(scr, t)
        c1 = c + ALPHA * (a + b)
        d1 = d + ALPHA * (b + up(a, 1, 2, b))
        a1 = a + BETA * (dn(d1, 1, 0, c1) + c1)
        b1 = b + BETA * (c1 + d1)
        c2 = c1 + GAMMA * (a1 + b1)
        d2 = d1 + GAMMA * (b1 + up(a1, 1, 3, b1))
        a = (a1 + DELTA * (dn(d2, 1, 1, c2) + c2)) * SCALE_LOW
        b = (b1 + DELTA * (c2 + d2)) * SCALE_LOW
        v_ref[t, 0] = a
        v_ref[t, 1] = b
        v_ref[t, 2] = c2 * SCALE_HIGH
        v_ref[t, 3] = d2 * SCALE_HIGH
        b1 = b + ALPHA * (a + up(a, 2, 2, a))
        a1 = a + BETA * (dn(b1, 2, 0, b1) + b1)
        b2 = b1 + GAMMA * (a1 + up(a1, 2, 3, a1))
        x = (a1 + DELTA * (dn(b2, 2, 1, b2) + b2)) * SCALE_LOW
        v_ref[t, 4] = x
        v_ref[t, 5] = b2 * SCALE_HIGH
        for co, ce, j in ((c_alpha, c_beta, 0), (c_gamma, c_delta, 1)):
            l = pltpu.roll(x, 1, 0)
            x = x + co * (l + up(x, 3, 2 + j, l))
            r = pltpu.roll(x, 7, 0)
            x = x + ce * (dn(x, 3, j, r) + r)
        v_ref[t, 6] = x * c_scale
        return carry

    for img in range(IMAGES):
        for rt in range(4):
            copies[img * 4 + rt].wait()
        lax.fori_loop(img * CHUNKS, (img + 1) * CHUNKS, body, 0)

    lane = lax.broadcasted_iota(jnp.int32, (8, LANES), 1)
    for n, (base, count, width) in enumerate(KINDS):
        to_left = zero
        to_right = zero
        for img in range(IMAGES):
            for q in range(count):
                slot = (img * count + q) * width
                here = (lane >= slot) & (lane < slot + width)
                start = v_ref[img * CHUNKS, base + q]
                end = v_ref[img * CHUNKS + CHUNKS - 1, base + q]
                if slot:
                    start = pltpu.roll(start, slot, 1)
                if (slot + width) % LANES:
                    end = pltpu.roll(end, slot + width, 1)
                to_left = jnp.where(here, start, to_left)
                to_right = jnp.where(here, end, to_right)
        left_ref[pl.ds(8 * n, 8), :] = to_left
        right_ref[pl.ds(8 * n, 8), :] = to_right


def cols_kernel(v_ref, from_left, from_right, out_ref, scr, halo, sems):
    col = lax.axis_index("col")
    first = col == 0
    last = col == lax.axis_size("col") - 1
    lane = lax.broadcasted_iota(jnp.int32, (8, LANES), 1)
    zero = jnp.zeros((8, LANES), jnp.float32)

    for n, (base, count, width) in enumerate(KINDS):
        got_l = from_left[pl.ds(8 * n, 8), :]
        got_r = from_right[pl.ds(8 * n, 8), :]
        for img in range(IMAGES):
            for q in range(count):
                slot = (img * count + q) * width
                halo[img, base + q, 0] = pltpu.roll(got_l, (LANES - slot - width) % LANES, 1) if (slot + width) % LANES else got_l
                halo[img, base + q, 1] = pltpu.roll(got_r, (LANES - slot) % LANES, 1) if slot else got_r

    def level_pass(xs, level):
        st = 1 << (level - 1)
        pos = lane & (2 * st - 1)
        co = pos == st
        ce = pos == 0
        hi_edge = lane >= LANES - st
        lo_edge = lane < st
        mir_hi = hi_edge & last
        mir_lo = lo_edge & first
        n = len(xs)
        for ka, kb in ((ALPHA, BETA), (GAMMA, DELTA)):
            ca = jnp.where(co, ka, zero)
            cb = jnp.where(ce, kb, zero)
            rights = [pltpu.roll(x, LANES - st, 1) for x in xs]
            lefts = [pltpu.roll(x, st, 1) for x in xs]
            new = []
            for i in range(n):
                r = rights[i]
                if i + 1 < n:
                    r = jnp.where(hi_edge, rights[i + 1], r)
                if i == n - 2:
                    r = jnp.where(mir_hi, lefts[i], r)
                new.append(xs[i] + ca * (lefts[i] + r))
            xs = new
            rights = [pltpu.roll(x, LANES - st, 1) for x in xs]
            lefts = [pltpu.roll(x, st, 1) for x in xs]
            new = []
            for i in range(n):
                l = lefts[i]
                if i:
                    l = jnp.where(lo_edge, lefts[i - 1], l)
                if i == 1:
                    l = jnp.where(mir_lo, rights[i], l)
                new.append(xs[i] + cb * (l + rights[i]))
            xs = new
        scale = jnp.where(co, SCALE_HIGH, SCALE_LOW).astype(jnp.float32)
        return [x * scale for x in xs]

    def line(img, k):
        return (
            [halo[img, k, 0]]
            + [v_ref[img * CHUNKS + c, k] for c in range(CHUNKS)]
            + [halo[img, k, 1]]
        )

    def put(img, q, keep, xs):
        for c in range(CHUNKS):
            where = (img * CHUNKS + c, pl.ds((q & 1) * 2 + (q >> 1), 8, stride=4), slice(None))
            val = xs[c + 1]
            if keep is not None:
                val = jnp.where(keep, val, scr[where])
            scr[where] = val

    def image(img, carry):
        def v1(q, carry):
            put(img, q, None, level_pass(line(img, q), 1))
            return carry

        lax.fori_loop(0, 4, v1, 0)

        def v2(q, carry):
            put(img, q, (lane & 1) == 0, level_pass(level_pass(line(img, 4 + q), 1), 2))
            return carry

        lax.fori_loop(0, 2, v2, 0)
        xs = line(img, 6)
        for level in (1, 2, 3):
            xs = level_pass(xs, level)
        put(img, 0, (lane & 3) == 0, xs)
        for rt in range(4):
            pltpu.make_async_copy(
                scr.at[pl.ds(img * CHUNKS, CHUNKS), pl.ds(rt * 8, 8), :], out_ref.at[img, rt], sems.at[img, rt]
            ).start()
        return carry

    for img in range(IMAGES):
        image(img, 0)
    for img in range(IMAGES):
        for rt in range(4):
            pltpu.make_async_copy(
                scr.at[pl.ds(img * CHUNKS, CHUNKS), pl.ds(rt * 8, 8), :], out_ref.at[img, rt], sems.at[img, rt]
            ).wait()


def _swaps(count):
    even = [(i, i ^ 1) for i in range(count)]
    odd = [(i, i + 1 if i % 2 else i - 1) for i in range(1, count - 1)] + [(0, count - 1), (count - 1, 0)]
    return even, odd


def exchange(axis, to_prev, to_next):
    even_pairs, odd_pairs = _swaps(lax.axis_size(axis))
    is_odd = lax.axis_index(axis) % 2 == 1
    via_even = lax.ppermute(jnp.where(is_odd, to_prev, to_next), axis, even_pairs)
    via_odd = lax.ppermute(jnp.where(is_odd, to_next, to_prev), axis, odd_pairs)
    from_prev = jnp.where(is_odd, via_even, via_odd)
    from_next = jnp.where(is_odd, via_odd, via_even)
    return from_prev, from_next


F32 = jnp.float32
VMEM = pl.BlockSpec(memory_space=pltpu.VMEM)
ANY = pl.BlockSpec(memory_space=pl.ANY)


def shards(images):
    x = images.reshape(IMAGES, 4, 8, CHUNKS, LANES).transpose(0, 1, 3, 2, 4)
    state = jax.ShapeDtypeStruct((6 * TILES, LANES), F32)
    end, start = pl.pallas_call(
        states_kernel,
        out_shape=(state, state),
        in_specs=[ANY],
        out_specs=(VMEM, VMEM),
        scratch_shapes=[pltpu.VMEM((TILES, ROWS, LANES), F32), pltpu.SemaphoreType.DMA((IMAGES, 4))],
        name="row_states",
    )(x)
    got_end, got_start = exchange("row", start, end)
    edge = jax.ShapeDtypeStruct((24, LANES), F32)
    v, to_left, to_right = pl.pallas_call(
        rows_kernel,
        out_shape=(jax.ShapeDtypeStruct((TILES, 7, 8, LANES), F32), edge, edge),
        in_specs=[ANY, VMEM, VMEM, VMEM, VMEM],
        out_specs=(VMEM, VMEM, VMEM),
        scratch_shapes=[
            pltpu.VMEM((TILES, ROWS, LANES), F32),
            pltpu.VMEM((12 * TILES, LANES), F32),
            pltpu.SemaphoreType.DMA((IMAGES, 4)),
        ],
        name="rows_all",
    )(x, end, start, got_end, got_start)
    from_left, from_right = exchange("col", to_left, to_right)
    out = pl.pallas_call(
        cols_kernel,
        out_shape=jax.ShapeDtypeStruct((IMAGES, 4, CHUNKS, 8, LANES), F32),
        in_specs=[VMEM, VMEM, VMEM],
        out_specs=ANY,
        scratch_shapes=[
            pltpu.VMEM((TILES, ROWS, LANES), F32),
            pltpu.VMEM((IMAGES, 7, 2, 8, LANES), F32),
            pltpu.SemaphoreType.DMA((IMAGES, 4)),
        ],
        name="cols_all",
    )(v, from_left, from_right)
    return out.transpose(0, 1, 3, 2, 4).reshape(IMAGES, ROWS, CHUNKS * LANES)


def solution(mesh):
    return jax.shard_map(
        shards,
        mesh=mesh,
        in_specs=(P(None, "row", "col"),),
        out_specs=P(None, "row", "col"),
        check_vma=False,
    )
```

```python
import jax
import jax.numpy as jnp
import numpy as np
from jax import lax
from jax.experimental import pallas as pl
from jax.experimental.pallas import tpu as pltpu
from jax.sharding import PartitionSpec as P

ALPHA = -1.586134342
BETA = -0.05298011854
GAMMA = 0.8829110762
DELTA = 0.4435068522
SCALE_HIGH = 1.230174105
SCALE_LOW = 1.0 / 1.230174105

IMAGES = 4
ROWS = 32
CHUNKS = 16
TILES = IMAGES * CHUNKS
LANES = 128
EDGES = 2 * IMAGES
HALF = LANES // 2
PATCH = 32
F32 = jnp.float32
OFFSETS = (0, 2, 1, 3)
KINDS = ((0, 4, 8), (4, 2, 16), (6, 1, 32))


def tile_row(img, chunk):
    place = 0 if chunk == 0 else 1 if chunk == CHUNKS - 1 else chunk + 1
    return place * IMAGES + img


def _lift(x, left, right):
    s, d = x[0::2], x[1::2]
    m = len(s)
    d = [d[i] + ALPHA * (s[i] + (s[i + 1] if i + 1 < m else right[0])) for i in range(m)]
    s = [s[i] + BETA * ((d[i - 1] if i else left[0]) + d[i]) for i in range(m)]
    d = [d[i] + GAMMA * (s[i] + (s[i + 1] if i + 1 < m else right[1])) for i in range(m)]
    s = [s[i] + DELTA * ((d[i - 1] if i else left[1]) + d[i]) for i in range(m)]
    return [v * SCALE_LOW for v in s], [v * SCALE_HIGH for v in d]


def _states(x):
    p = x[-1] + ALPHA * x[-2]
    t = x[-2] + BETA * (x[-3] + ALPHA * (x[-4] + x[-2]))
    s = x[0]
    u = x[0] + BETA * (x[1] + ALPHA * (x[0] + x[2]))
    return p, t, s, u


def _responses():
    zero = (0.0, 0.0)
    end, start = {}, {}
    for level in (1, 2):
        for j in range(2):
            unit = (1.0, 0.0) if j == 0 else (0.0, 1.0)
            for table, left, right, pick in ((end, zero, unit, 0), (start, unit, zero, 2)):
                band = [0.0] * (ROWS >> (level - 1))
                low, _ = _lift(band, left, right)
                for into in range(level + 1, 4):
                    table[level, into, j] = _states(low)[pick : pick + 2]
                    low, _ = _lift(low, zero, zero)
    return end, start


def _taps():
    low, high = [0.0] * 9, [0.0] * 9
    for k in range(-4, 5):
        x = [0.0] * 64
        x[32 + k] = 1.0
        low[k + 4] = _lift(x, (0.0, 0.0), (0.0, 0.0))[0][16]
        x = [0.0] * 64
        x[33 + k] = 1.0
        high[k + 4] = _lift(x, (0.0, 0.0), (0.0, 0.0))[1][16]
    return low, high


END, START = _responses()
LOW, HIGH = _taps()


def _edge_taps():
    table = np.zeros((2, 2, 3, 9, LANES), np.float32)
    for side in range(2):
        for mirrored in range(2):
            for level in range(3):
                st = 1 << level
                for lane in range(0, LANES, st):
                    taps = HIGH if (lane // st) % 2 else LOW
                    for k in range(-4, 5):
                        target = lane + k * st
                        if mirrored and side == 0 and target < HALF <= lane:
                            target = 2 * HALF - target
                        edge = HALF - st
                        if mirrored and side == 1 and target > edge >= lane:
                            target = 2 * edge - target
                        table[side, mirrored, level, (target - lane) // st + 4, lane] += taps[k + 4]
    return table.reshape(2 * 2, 27, LANES)


EDGE_TAPS = _edge_taps()


def _sub():
    return lax.broadcasted_iota(jnp.int32, (8, LANES), 0)


def _lane():
    return lax.broadcasted_iota(jnp.int32, (8, LANES), 1)


def _load(src, dst, sem):
    copy = pltpu.make_async_copy(src, dst, sem)
    copy.start()
    return copy


def _rows_of(ref, t):
    return [ref[t, pl.ds(q, 8, stride=4), :] for q in OFFSETS]


def _states_of(tile):
    sub = _sub()
    is7, is0 = sub == 7, sub == 0
    zero = jnp.zeros((8, LANES), F32)

    def up(v):
        return jnp.where(is7, zero, pltpu.roll(v, 7, 0))

    def dn(v):
        return jnp.where(is0, zero, pltpu.roll(v, 1, 0))

    a, b, c, d = tile
    c1 = c + ALPHA * (a + b)
    end = [(d + ALPHA * b)[7:8], (b + BETA * c1)[7:8]]
    start = [a[0:1], (a + BETA * c1)[0:1]]
    d1 = d + ALPHA * (b + up(a))
    a1 = a + BETA * (dn(d1) + c1)
    b1 = b + BETA * (c1 + d1)
    c2 = c1 + GAMMA * (a1 + b1)
    d2 = d1 + GAMMA * (b1 + up(a1))
    a = (a1 + DELTA * (dn(d2) + c2)) * SCALE_LOW
    b = (b1 + DELTA * (c2 + d2)) * SCALE_LOW
    b1 = b + ALPHA * (a + up(a))
    rb = dn(b1)
    end += [(b + ALPHA * a)[7:8], (a + BETA * rb)[7:8]]
    start += [a[0:1], (a + BETA * b1)[0:1]]
    a1 = a + BETA * (rb + b1)
    b2 = b1 + GAMMA * (a1 + up(a1))
    x = (a1 + DELTA * (dn(b2) + b2)) * SCALE_LOW
    back = pltpu.roll(x, 1, 0)
    x1 = x + ALPHA * (back + pltpu.roll(x, 7, 0))
    end += [(x + ALPHA * back)[7:8], (x + BETA * pltpu.roll(x1, 1, 0))[6:7]]
    start += [x[0:1], (x + BETA * pltpu.roll(x1, 7, 0))[0:1]]
    return end, start


def _junction(ends, starts):
    out = []
    for level in (1, 2, 3):
        p, t = ends[2 * level - 2], ends[2 * level - 1]
        s, u = starts[2 * level - 2], starts[2 * level - 1]
        for prior in range(1, level):
            l1, l2, r1, r2 = out[prior - 1]
            e0, e1 = END[prior, level, 0], END[prior, level, 1]
            s0, s1 = START[prior, level, 0], START[prior, level, 1]
            p = p + e0[0] * r1 + e1[0] * r2
            t = t + e0[1] * r1 + e1[1] * r2
            s = s + s0[0] * l1 + s1[0] * l2
            u = u + s0[1] * l1 + s1[1] * l2
        l1 = p + ALPHA * s
        r2 = u + BETA * l1
        l2 = l1 + GAMMA * (t + BETA * l1 + r2)
        out.append((l1, l2, s, r2))
    return out


def _boundaries(own_even, own_odd, got_even, got_odd, bnd, count):
    odd = lax.axis_index("row") % 2 == 1

    def read(ref):
        return [ref[pl.ds(k * TILES, count), :] for k in range(6)]

    oe, oo, ge, go = read(own_even), read(own_odd), read(got_even), read(got_odd)

    def pick(yes, no):
        return [jnp.where(odd, y, n) for y, n in zip(yes, no)]

    top = _junction(pick(ge, go), pick(oe, oo))
    low = _junction(pick(oo, oe), pick(go, ge))
    for level in range(3):
        for j in range(4):
            bnd[pl.ds((level * 4 + j) * count, count), :] = (top if j < 2 else low)[level][j]


def _rows_transform(tile, edge):
    row = lax.axis_index("row")
    sub = _sub()
    is7, is0 = sub == 7, sub == 0
    mir7 = is7 & (row == lax.axis_size("row") - 1)
    mir0 = is0 & (row == 0)
    odd = (sub & 1) == 1
    zero = jnp.zeros((8, LANES), F32)

    def up(v, level, j, mirror):
        return jnp.where(mir7, mirror, jnp.where(is7, edge(level, j), pltpu.roll(v, 7, 0)))

    def dn(v, level, j, mirror):
        return jnp.where(mir0, mirror, jnp.where(is0, edge(level, j), pltpu.roll(v, 1, 0)))

    a, b, c, d = tile
    c1 = c + ALPHA * (a + b)
    d1 = d + ALPHA * (b + up(a, 0, 2, b))
    a1 = a + BETA * (dn(d1, 0, 0, c1) + c1)
    b1 = b + BETA * (c1 + d1)
    c2 = c1 + GAMMA * (a1 + b1)
    d2 = d1 + GAMMA * (b1 + up(a1, 0, 3, b1))
    a = (a1 + DELTA * (dn(d2, 0, 1, c2) + c2)) * SCALE_LOW
    b = (b1 + DELTA * (c2 + d2)) * SCALE_LOW
    v = [a, b, c2 * SCALE_HIGH, d2 * SCALE_HIGH]
    b1 = b + ALPHA * (a + up(a, 1, 2, a))
    a1 = a + BETA * (dn(b1, 1, 0, b1) + b1)
    b2 = b1 + GAMMA * (a1 + up(a1, 1, 3, a1))
    x = (a1 + DELTA * (dn(b2, 1, 1, b2) + b2)) * SCALE_LOW
    v += [x, b2 * SCALE_HIGH]
    for ka, kb, j in ((ALPHA, BETA, 0), (GAMMA, DELTA, 1)):
        back = pltpu.roll(x, 1, 0)
        x = x + jnp.where(odd, ka, zero) * (back + up(x, 2, 2 + j, back))
        ahead = pltpu.roll(x, 7, 0)
        x = x + jnp.where(odd, zero, kb) * (dn(x, 2, j, ahead) + ahead)
    v.append(x * jnp.where(odd, SCALE_HIGH, zero + SCALE_LOW))
    return v


def states_kernel(x_ref, even_ref, odd_ref, scr, sems):
    copies = [
        [
            _load(
                x_ref.at[img, rt],
                scr.at[pl.ds(img * CHUNKS, CHUNKS), pl.ds(rt * 8, 8), :],
                sems.at[img, rt],
            )
            for rt in range(4)
        ]
        for img in range(IMAGES)
    ]
    is_odd = lax.axis_index("row") % 2 == 1
    for img in range(IMAGES):
        for copy in copies[img]:
            copy.wait()
        for group in range(0, CHUNKS, 4):
            got = [
                (tile_row(img, c), *_states_of(_rows_of(scr, img * CHUNKS + c))) for c in range(group, group + 4)
            ]

            def put(to_end, to_start):
                for t, end, start in got:
                    for k in range(6):
                        to_end[pl.ds(k * TILES + t, 1), :] = end[k]
                        to_start[pl.ds(k * TILES + t, 1), :] = start[k]

            pl.when(is_odd)(lambda: put(odd_ref, even_ref))
            pl.when(jnp.logical_not(is_odd))(lambda: put(even_ref, odd_ref))


def edges_kernel(x_ref, own_even, own_odd, got_even, got_odd, v_ref, even_ref, odd_ref, scr, bnd, sems):
    copies = []
    for side, chunk in enumerate((0, CHUNKS - 1)):
        for img in range(IMAGES):
            for rt in range(4):
                copies.append(
                    _load(
                        x_ref.at[img, rt, chunk],
                        scr.at[side * IMAGES + img, pl.ds(rt * 8, 8), :],
                        sems.at[side * IMAGES + img, rt],
                    )
                )
    _boundaries(own_even, own_odd, got_even, got_odd, bnd, EDGES)
    for copy in copies:
        copy.wait()
    lane = _lane()
    zero = jnp.zeros((8, LANES), F32)
    tiles = []
    for t in range(EDGES):

        def edge(level, j, t=t):
            return jnp.broadcast_to(bnd[pl.ds((level * 4 + j) * EDGES + t, 1), :], (8, LANES))

        v = _rows_transform(_rows_of(scr, t), edge)
        for k in range(7):
            v_ref[t, k] = v[k]
        tiles.append(v)
    is_odd = lax.axis_index("col") % 2 == 1
    for n, (base, count, width) in enumerate(KINDS):
        to_left, to_right = zero, zero
        for img in range(IMAGES):
            for q in range(count):
                slot = (img * count + q) * width
                here = (lane >= slot) & (lane < slot + width)
                start, end = tiles[img][base + q], tiles[IMAGES + img][base + q]
                if slot:
                    start = pltpu.roll(start, slot, 1)
                if (slot + width) % LANES:
                    end = pltpu.roll(end, slot + width, 1)
                to_left = jnp.where(here, start, to_left)
                to_right = jnp.where(here, end, to_right)
        even_ref[pl.ds(8 * n, 8), :] = jnp.where(is_odd, to_left, to_right)
        odd_ref[pl.ds(8 * n, 8), :] = jnp.where(is_odd, to_right, to_left)


def main_kernel(x_ref, own_even, own_odd, got_even, got_odd, out_ref, edge_ref, scr, vs, bnd, in_sems, out_sems):
    copies = [
        [
            _load(
                x_ref.at[img, rt],
                scr.at[pl.ds(img * CHUNKS, CHUNKS), pl.ds(rt * 8, 8), :],
                in_sems.at[img, rt],
            )
            for rt in range(4)
        ]
        for img in range(IMAGES)
    ]
    _boundaries(own_even, own_odd, got_even, got_odd, bnd, TILES)
    lane = _lane()

    def band_pass(xs, level):
        st = 1 << level
        pos = lane & (2 * st - 1)
        is_low, is_high = pos == 0, pos == st
        rolls = [
            {k: pltpu.roll(x, (k * st) % LANES, 1) for k in (-4, -3, -2, -1, 1, 2, 3, 4)} for x in xs
        ]
        coefs = [jnp.where(is_low, LOW[4 + k], jnp.where(is_high, HIGH[4 + k], 0.0)).astype(F32) for k in range(5)]
        out = []
        for c in range(CHUNKS):
            acc = coefs[0] * xs[c]
            for k in range(1, 5):
                before, after = rolls[c][k], rolls[c][-k]
                if c:
                    before = jnp.where(lane < k * st, rolls[c - 1][k], before)
                if c < CHUNKS - 1:
                    after = jnp.where(lane >= LANES - k * st, rolls[c + 1][-k], after)
                acc = acc + coefs[k] * (before + after)
            out.append(acc)
        return out

    def line(k):
        return [vs[k, c] for c in range(CHUNKS)]

    def image(img):
        for c in range(CHUNKS):

            def edge(level, j, c=c):
                t = tile_row(img, c)
                return jnp.broadcast_to(bnd[pl.ds((level * 4 + j) * TILES + t, 1), :], (8, LANES))

            v = _rows_transform(_rows_of(scr, img * CHUNKS + c), edge)
            for k in range(7):
                vs[k, c] = v[k]

        def put(k, keep, xs):
            for c in range(CHUNKS):
                where = (img * CHUNKS + c, pl.ds(OFFSETS[k], 8, stride=4), slice(None))
                scr[where] = xs[c] if keep is None else jnp.where(keep, xs[c], scr[where])

        for k in range(4):
            put(k, None, band_pass(line(k), 0))
        for k in range(2):
            put(k, (lane & 1) == 0, band_pass(band_pass(line(4 + k), 0), 1))
        put(0, (lane & 3) == 0, band_pass(band_pass(band_pass(line(6), 0), 1), 2))
        for side, chunk in enumerate((0, CHUNKS - 1)):
            edge_ref[side * IMAGES + img] = scr[img * CHUNKS + chunk]

    stores = []
    for img in range(IMAGES):
        for copy in copies[img]:
            copy.wait()
        image(img)
        for rt in range(4):
            stores.append(
                _load(
                    scr.at[pl.ds(img * CHUNKS + 1, CHUNKS - 2), pl.ds(rt * 8, 8), :],
                    out_ref.at[img, rt, pl.ds(1, CHUNKS - 2)],
                    out_sems.at[img, rt],
                )
            )
    for copy in stores:
        copy.wait()


def patch_kernel(taps_ref, v_ref, edge_in, got_even, got_odd, dest_ref, out_ref, scr, sems):
    del dest_ref
    col = lax.axis_index("col")
    is_odd = col % 2 == 1
    at_edge = (jnp.where(col == 0, 1, 0), jnp.where(col == lax.axis_size("col") - 1, 1, 0))
    lane = _lane()
    low_half = lane < HALF
    windows = ([], [])
    for n, (base, count, width) in enumerate(KINDS):
        via_even, via_odd = got_even[pl.ds(8 * n, 8), :], got_odd[pl.ds(8 * n, 8), :]
        got = (jnp.where(is_odd, via_even, via_odd), jnp.where(is_odd, via_odd, via_even))
        for img in range(IMAGES):
            for q in range(count):
                slot = (img * count + q) * width
                for side, shift in ((0, HALF - slot - width), (1, HALF - slot)):
                    halo = pltpu.roll(got[side], shift % LANES, 1) if shift % LANES else got[side]
                    own = pltpu.roll(v_ref[side * IMAGES + img, base + q], HALF, 1)
                    first, second = (halo, own) if side == 0 else (own, halo)
                    windows[side].append((img, base + q, jnp.where(low_half, first, second)))

    def band_pass(xs, side, level):
        row = side * 2 + at_edge[side]
        coefs = [
            jnp.broadcast_to(taps_ref[row, pl.ds(level * 9 + k, 1), :], (8, LANES)) for k in range(9)
        ]
        st = 1 << level
        out = []
        for x in xs:
            acc = coefs[4] * x
            for k in (-4, -3, -2, -1, 1, 2, 3, 4):
                acc = acc + coefs[4 + k] * pltpu.roll(x, (-k * st) % LANES, 1)
            out.append(acc)
        return out

    copies = []
    for side in range(2):
        keys = [(img, k) for img, k, _ in windows[side]]
        xs = band_pass([w for _, _, w in windows[side]], side, 0)
        done = dict(zip(keys, xs))
        deeper = [key for key in keys if key[1] >= 4]
        done.update(zip(deeper, band_pass([done[key] for key in deeper], side, 1)))
        deepest = [key for key in keys if key[1] >= 6]
        done.update(zip(deepest, band_pass([done[key] for key in deepest], side, 2)))
        inside = lane < PATCH if side == 0 else lane >= LANES - PATCH
        for img in range(IMAGES):
            t = side * IMAGES + img
            for q in range(4):
                new = done[img, q]
                if q < 2:
                    new = jnp.where((lane & 1) == 0, done[img, 4 + q], new)
                if q < 1:
                    new = jnp.where((lane & 3) == 0, done[img, 6], new)
                where = (t, pl.ds(OFFSETS[q], 8, stride=4), slice(None))
                scr[where] = jnp.where(inside, pltpu.roll(new, HALF, 1), edge_in[where])
            for rt in range(4):
                copies.append(
                    _load(
                        scr.at[t, pl.ds(rt * 8, 8), :],
                        out_ref.at[img, rt, (CHUNKS - 1) * side],
                        sems.at[t, rt],
                    )
                )
    for copy in copies:
        copy.wait()


def swap(axis, even, odd):
    n = lax.axis_size(axis)
    even_pairs = [(i, i ^ 1) for i in range(n)]
    odd_pairs = [(i, (i + 1 if i % 2 else i - 1) % n) for i in range(n)]
    return lax.ppermute(even, axis, even_pairs), lax.ppermute(odd, axis, odd_pairs)


VMEM = pl.BlockSpec(memory_space=pltpu.VMEM)
ANY = pl.BlockSpec(memory_space=pl.ANY)


def shape(*dims):
    return jax.ShapeDtypeStruct(dims, F32)


def shards(images):
    x = images.reshape(IMAGES, 4, 8, CHUNKS, LANES).transpose(0, 1, 3, 2, 4)
    dma = pltpu.SemaphoreType.DMA
    row_even, row_odd = pl.pallas_call(
        states_kernel,
        out_shape=(shape(6 * TILES, LANES), shape(6 * TILES, LANES)),
        in_specs=[ANY],
        out_specs=(VMEM, VMEM),
        scratch_shapes=[pltpu.VMEM((TILES, ROWS, LANES), F32), dma((IMAGES, 4))],
        name="row_states",
    )(x)
    got_even, got_odd = swap("row", row_even, row_odd)
    rows = (row_even, row_odd, got_even, got_odd)
    v_edge, col_even, col_odd = pl.pallas_call(
        edges_kernel,
        out_shape=(shape(EDGES, 7, 8, LANES), shape(24, LANES), shape(24, LANES)),
        in_specs=[ANY] + [VMEM] * 4,
        out_specs=(VMEM,) * 3,
        scratch_shapes=[
            pltpu.VMEM((EDGES, ROWS, LANES), F32),
            pltpu.VMEM((12 * EDGES, LANES), F32),
            dma((EDGES, 4)),
        ],
        name="edge_rows",
    )(x, *rows)
    halo_even, halo_odd = swap("col", col_even, col_odd)
    out, out_edge = pl.pallas_call(
        main_kernel,
        out_shape=(shape(IMAGES, 4, CHUNKS, 8, LANES), shape(EDGES, ROWS, LANES)),
        in_specs=[ANY] + [VMEM] * 4,
        out_specs=(ANY, VMEM),
        scratch_shapes=[
            pltpu.VMEM((TILES, ROWS, LANES), F32),
            pltpu.VMEM((7, CHUNKS, 8, LANES), F32),
            pltpu.VMEM((12 * TILES, LANES), F32),
            dma((IMAGES, 4)),
            dma((IMAGES, 4)),
        ],
        cost_estimate=pl.CostEstimate(flops=40_000_000, transcendentals=0, bytes_accessed=2_000_000),
        name="interior",
    )(x, *rows)
    out = pl.pallas_call(
        patch_kernel,
        out_shape=shape(IMAGES, 4, CHUNKS, 8, LANES),
        in_specs=[VMEM] * 5 + [ANY],
        out_specs=ANY,
        input_output_aliases={5: 0},
        scratch_shapes=[pltpu.VMEM((EDGES, ROWS, LANES), F32), dma((EDGES, 4))],
        name="edge_columns",
    )(jnp.asarray(EDGE_TAPS), v_edge, out_edge, halo_even, halo_odd, out)
    return out.transpose(0, 1, 3, 2, 4).reshape(IMAGES, ROWS, CHUNKS * LANES)


def solution(mesh):
    return jax.shard_map(
        shards,
        mesh=mesh,
        in_specs=(P(None, "row", "col"),),
        out_specs=P(None, "row", "col"),
        check_vma=False,
    )
```

```python
import jax
import jax.numpy as jnp
import numpy as np
from jax import lax
from jax.experimental import pallas as pl
from jax.experimental.pallas import tpu as pltpu
from jax.sharding import PartitionSpec as P


ALPHA = -1.586134342
BETA = -0.05298011854
GAMMA = 0.8829110762
DELTA = 0.4435068522
SCALE_HIGH = 1.230174105
SCALE_LOW = 1.0 / 1.230174105

IMAGES = 4
ROWS = 32
CHUNKS = 16
TILES = IMAGES * CHUNKS
LANES = 128
EDGES = 2 * IMAGES
HALF = LANES // 2
PATCH = 32
F32 = jnp.float32
OFFSETS = (0, 2, 1, 3)
KINDS = ((0, 4, 8), (4, 2, 16), (6, 1, 32))


def tile_row(img, chunk):
    place = 0 if chunk == 0 else 1 if chunk == CHUNKS - 1 else chunk + 1
    return place * IMAGES + img


def _lift(x, left, right):
    s, d = x[0::2], x[1::2]
    m = len(s)
    d = [d[i] + ALPHA * (s[i] + (s[i + 1] if i + 1 < m else right[0])) for i in range(m)]
    s = [s[i] + BETA * ((d[i - 1] if i else left[0]) + d[i]) for i in range(m)]
    d = [d[i] + GAMMA * (s[i] + (s[i + 1] if i + 1 < m else right[1])) for i in range(m)]
    s = [s[i] + DELTA * ((d[i - 1] if i else left[1]) + d[i]) for i in range(m)]
    return [v * SCALE_LOW for v in s], [v * SCALE_HIGH for v in d]


def _states(x):
    p = x[-1] + ALPHA * x[-2]
    t = x[-2] + BETA * (x[-3] + ALPHA * (x[-4] + x[-2]))
    s = x[0]
    u = x[0] + BETA * (x[1] + ALPHA * (x[0] + x[2]))
    return p, t, s, u


def _responses():
    zero = (0.0, 0.0)
    end, start = {}, {}
    for level in (1, 2):
        for j in range(2):
            unit = (1.0, 0.0) if j == 0 else (0.0, 1.0)
            for table, left, right, pick in ((end, zero, unit, 0), (start, unit, zero, 2)):
                band = [0.0] * (ROWS >> (level - 1))
                low, _ = _lift(band, left, right)
                for into in range(level + 1, 4):
                    table[level, into, j] = _states(low)[pick : pick + 2]
                    low, _ = _lift(low, zero, zero)
    return end, start


def _taps():
    low, high = [0.0] * 9, [0.0] * 9
    for k in range(-4, 5):
        x = [0.0] * 64
        x[32 + k] = 1.0
        low[k + 4] = _lift(x, (0.0, 0.0), (0.0, 0.0))[0][16]
        x = [0.0] * 64
        x[33 + k] = 1.0
        high[k + 4] = _lift(x, (0.0, 0.0), (0.0, 0.0))[1][16]
    return low, high


END, START = _responses()
LOW, HIGH = _taps()


def _edge_taps():
    table = np.zeros((2, 2, 3, 9, LANES), np.float32)
    for side in range(2):
        for mirrored in range(2):
            for level in range(3):
                st = 1 << level
                for lane in range(0, LANES, st):
                    taps = HIGH if (lane // st) % 2 else LOW
                    for k in range(-4, 5):
                        target = lane + k * st
                        if mirrored and side == 0 and target < HALF <= lane:
                            target = 2 * HALF - target
                        edge = HALF - st
                        if mirrored and side == 1 and target > edge >= lane:
                            target = 2 * edge - target
                        table[side, mirrored, level, (target - lane) // st + 4, lane] += taps[k + 4]
    return table.reshape(2 * 2, 27, LANES)


EDGE_TAPS = _edge_taps()


def _sub():
    return lax.broadcasted_iota(jnp.int32, (8, LANES), 0)


def _lane():
    return lax.broadcasted_iota(jnp.int32, (8, LANES), 1)


def _load(src, dst, sem):
    copy = pltpu.make_async_copy(src, dst, sem)
    copy.start()
    return copy


def _rows_of(ref, t):
    return [ref[t, pl.ds(q, 8, stride=4), :] for q in OFFSETS]


def _states_of(tile):
    sub = _sub()
    is7, is0 = sub == 7, sub == 0
    zero = jnp.zeros((8, LANES), F32)

    def up(v):
        return jnp.where(is7, zero, pltpu.roll(v, 7, 0))

    def dn(v):
        return jnp.where(is0, zero, pltpu.roll(v, 1, 0))

    a, b, c, d = tile
    c1 = c + ALPHA * (a + b)
    end = [(d + ALPHA * b)[7:8], (b + BETA * c1)[7:8]]
    start = [a[0:1], (a + BETA * c1)[0:1]]
    d1 = d + ALPHA * (b + up(a))
    a1 = a + BETA * (dn(d1) + c1)
    b1 = b + BETA * (c1 + d1)
    c2 = c1 + GAMMA * (a1 + b1)
    d2 = d1 + GAMMA * (b1 + up(a1))
    a = (a1 + DELTA * (dn(d2) + c2)) * SCALE_LOW
    b = (b1 + DELTA * (c2 + d2)) * SCALE_LOW
    b1 = b + ALPHA * (a + up(a))
    rb = dn(b1)
    end += [(b + ALPHA * a)[7:8], (a + BETA * rb)[7:8]]
    start += [a[0:1], (a + BETA * b1)[0:1]]
    a1 = a + BETA * (rb + b1)
    b2 = b1 + GAMMA * (a1 + up(a1))
    x = (a1 + DELTA * (dn(b2) + b2)) * SCALE_LOW
    back = pltpu.roll(x, 1, 0)
    x1 = x + ALPHA * (back + pltpu.roll(x, 7, 0))
    end += [(x + ALPHA * back)[7:8], (x + BETA * pltpu.roll(x1, 1, 0))[6:7]]
    start += [x[0:1], (x + BETA * pltpu.roll(x1, 7, 0))[0:1]]
    return end, start


def _junction(ends, starts):
    out = []
    for level in (1, 2, 3):
        p, t = ends[2 * level - 2], ends[2 * level - 1]
        s, u = starts[2 * level - 2], starts[2 * level - 1]
        for prior in range(1, level):
            l1, l2, r1, r2 = out[prior - 1]
            e0, e1 = END[prior, level, 0], END[prior, level, 1]
            s0, s1 = START[prior, level, 0], START[prior, level, 1]
            p = p + e0[0] * r1 + e1[0] * r2
            t = t + e0[1] * r1 + e1[1] * r2
            s = s + s0[0] * l1 + s1[0] * l2
            u = u + s0[1] * l1 + s1[1] * l2
        l1 = p + ALPHA * s
        r2 = u + BETA * l1
        l2 = l1 + GAMMA * (t + BETA * l1 + r2)
        out.append((l1, l2, s, r2))
    return out


def _boundaries(own_even, own_odd, got_even, got_odd, bnd, count):
    odd = lax.axis_index("row") % 2 == 1

    def read(ref):
        return [ref[pl.ds(k * TILES, count), :] for k in range(6)]

    oe, oo, ge, go = read(own_even), read(own_odd), read(got_even), read(got_odd)

    def pick(yes, no):
        return [jnp.where(odd, y, n) for y, n in zip(yes, no)]

    top = _junction(pick(ge, go), pick(oe, oo))
    low = _junction(pick(oo, oe), pick(go, ge))
    for level in range(3):
        for j in range(4):
            bnd[pl.ds((level * 4 + j) * count, count), :] = (top if j < 2 else low)[level][j]


def _rows_transform(tile, edge):
    row = lax.axis_index("row")
    sub = _sub()
    is7, is0 = sub == 7, sub == 0
    mir7 = is7 & (row == lax.axis_size("row") - 1)
    mir0 = is0 & (row == 0)
    odd = (sub & 1) == 1
    zero = jnp.zeros((8, LANES), F32)

    def up(v, level, j, mirror):
        return jnp.where(mir7, mirror, jnp.where(is7, edge(level, j), pltpu.roll(v, 7, 0)))

    def dn(v, level, j, mirror):
        return jnp.where(mir0, mirror, jnp.where(is0, edge(level, j), pltpu.roll(v, 1, 0)))

    a, b, c, d = tile
    c1 = c + ALPHA * (a + b)
    d1 = d + ALPHA * (b + up(a, 0, 2, b))
    a1 = a + BETA * (dn(d1, 0, 0, c1) + c1)
    b1 = b + BETA * (c1 + d1)
    c2 = c1 + GAMMA * (a1 + b1)
    d2 = d1 + GAMMA * (b1 + up(a1, 0, 3, b1))
    a = (a1 + DELTA * (dn(d2, 0, 1, c2) + c2)) * SCALE_LOW
    b = (b1 + DELTA * (c2 + d2)) * SCALE_LOW
    v = [a, b, c2 * SCALE_HIGH, d2 * SCALE_HIGH]
    b1 = b + ALPHA * (a + up(a, 1, 2, a))
    a1 = a + BETA * (dn(b1, 1, 0, b1) + b1)
    b2 = b1 + GAMMA * (a1 + up(a1, 1, 3, a1))
    x = (a1 + DELTA * (dn(b2, 1, 1, b2) + b2)) * SCALE_LOW
    v += [x, b2 * SCALE_HIGH]
    for ka, kb, j in ((ALPHA, BETA, 0), (GAMMA, DELTA, 1)):
        back = pltpu.roll(x, 1, 0)
        x = x + jnp.where(odd, ka, zero) * (back + up(x, 2, 2 + j, back))
        ahead = pltpu.roll(x, 7, 0)
        x = x + jnp.where(odd, zero, kb) * (dn(x, 2, j, ahead) + ahead)
    v.append(x * jnp.where(odd, SCALE_HIGH, zero + SCALE_LOW))
    return v


def states_kernel(x_ref, even_ref, odd_ref, scr, sems):
    copies = [
        [
            _load(
                x_ref.at[img, rt],
                scr.at[pl.ds(img * CHUNKS, CHUNKS), pl.ds(rt * 8, 8), :],
                sems.at[img, rt],
            )
            for rt in range(4)
        ]
        for img in range(IMAGES)
    ]
    is_odd = lax.axis_index("row") % 2 == 1
    for img in range(IMAGES):
        for copy in copies[img]:
            copy.wait()
        for group in range(0, CHUNKS, 4):
            got = [
                (tile_row(img, c), *_states_of(_rows_of(scr, img * CHUNKS + c))) for c in range(group, group + 4)
            ]

            def put(to_end, to_start):
                for t, end, start in got:
                    for k in range(6):
                        to_end[pl.ds(k * TILES + t, 1), :] = end[k]
                        to_start[pl.ds(k * TILES + t, 1), :] = start[k]

            pl.when(is_odd)(lambda: put(odd_ref, even_ref))
            pl.when(jnp.logical_not(is_odd))(lambda: put(even_ref, odd_ref))


def edges_kernel(x_ref, own_even, own_odd, got_even, got_odd, v_ref, even_ref, odd_ref, bnd):
    _boundaries(own_even, own_odd, got_even, got_odd, bnd, EDGES)
    lane = _lane()
    zero = jnp.zeros((8, LANES), F32)
    tiles = []
    for t in range(EDGES):

        def edge(level, j, t=t):
            return jnp.broadcast_to(bnd[pl.ds((level * 4 + j) * EDGES + t, 1), :], (8, LANES))

        column = (t % IMAGES) * CHUNKS + (t // IMAGES) * (CHUNKS - 1)
        v = _rows_transform(_rows_of(x_ref, column), edge)
        for k in range(7):
            v_ref[t, k] = v[k]
        tiles.append(v)
    is_odd = lax.axis_index("col") % 2 == 1
    for n, (base, count, width) in enumerate(KINDS):
        to_left, to_right = zero, zero
        for img in range(IMAGES):
            for q in range(count):
                slot = (img * count + q) * width
                here = (lane >= slot) & (lane < slot + width)
                start, end = tiles[img][base + q], tiles[IMAGES + img][base + q]
                if slot:
                    start = pltpu.roll(start, slot, 1)
                if (slot + width) % LANES:
                    end = pltpu.roll(end, slot + width, 1)
                to_left = jnp.where(here, start, to_left)
                to_right = jnp.where(here, end, to_right)
        even_ref[pl.ds(8 * n, 8), :] = jnp.where(is_odd, to_left, to_right)
        odd_ref[pl.ds(8 * n, 8), :] = jnp.where(is_odd, to_right, to_left)


def main_kernel(x_ref, own_even, own_odd, got_even, got_odd, out_ref, edge_ref, scr, vs, bnd, sems):
    _boundaries(own_even, own_odd, got_even, got_odd, bnd, TILES)
    lane = _lane()

    def band_pass(xs, level):
        st = 1 << level
        pos = lane & (2 * st - 1)
        is_low, is_high = pos == 0, pos == st
        rolls = [
            {k: pltpu.roll(x, (k * st) % LANES, 1) for k in (-4, -3, -2, -1, 1, 2, 3, 4)} for x in xs
        ]
        coefs = [jnp.where(is_low, LOW[4 + k], jnp.where(is_high, HIGH[4 + k], 0.0)).astype(F32) for k in range(5)]
        out = []
        for c in range(CHUNKS):
            acc = coefs[0] * xs[c]
            for k in range(1, 5):
                before, after = rolls[c][k], rolls[c][-k]
                if c:
                    before = jnp.where(lane < k * st, rolls[c - 1][k], before)
                if c < CHUNKS - 1:
                    after = jnp.where(lane >= LANES - k * st, rolls[c + 1][-k], after)
                acc = acc + coefs[k] * (before + after)
            out.append(acc)
        return out

    def line(k):
        return [vs[k, c] for c in range(CHUNKS)]

    def image(img):
        for c in range(CHUNKS):

            def edge(level, j, c=c):
                t = tile_row(img, c)
                return jnp.broadcast_to(bnd[pl.ds((level * 4 + j) * TILES + t, 1), :], (8, LANES))

            v = _rows_transform(_rows_of(x_ref, img * CHUNKS + c), edge)
            for k in range(7):
                vs[k, c] = v[k]

        def put(k, keep, xs):
            for c in range(CHUNKS):
                where = (img * CHUNKS + c, pl.ds(OFFSETS[k], 8, stride=4), slice(None))
                scr[where] = xs[c] if keep is None else jnp.where(keep, xs[c], scr[where])

        for k in range(4):
            put(k, None, band_pass(line(k), 0))
        for k in range(2):
            put(k, (lane & 1) == 0, band_pass(band_pass(line(4 + k), 0), 1))
        put(0, (lane & 3) == 0, band_pass(band_pass(band_pass(line(6), 0), 1), 2))
        for side, chunk in enumerate((0, CHUNKS - 1)):
            edge_ref[side * IMAGES + img] = scr[img * CHUNKS + chunk]

    stores = []
    for img in range(IMAGES):
        image(img)
        for rt in range(4):
            stores.append(
                _load(
                    scr.at[pl.ds(img * CHUNKS + 1, CHUNKS - 2), pl.ds(rt * 8, 8), :],
                    out_ref.at[img, rt, pl.ds(1, CHUNKS - 2)],
                    sems.at[img, rt],
                )
            )
    for copy in stores:
        copy.wait()


def patch_kernel(taps_ref, v_ref, edge_in, got_even, got_odd, dest_ref, out_ref, scr, sems):
    del dest_ref
    col = lax.axis_index("col")
    is_odd = col % 2 == 1
    at_edge = (jnp.where(col == 0, 1, 0), jnp.where(col == lax.axis_size("col") - 1, 1, 0))
    lane = _lane()
    low_half = lane < HALF
    windows = ([], [])
    for n, (base, count, width) in enumerate(KINDS):
        via_even, via_odd = got_even[pl.ds(8 * n, 8), :], got_odd[pl.ds(8 * n, 8), :]
        got = (jnp.where(is_odd, via_even, via_odd), jnp.where(is_odd, via_odd, via_even))
        for img in range(IMAGES):
            for q in range(count):
                slot = (img * count + q) * width
                for side, shift in ((0, HALF - slot - width), (1, HALF - slot)):
                    halo = pltpu.roll(got[side], shift % LANES, 1) if shift % LANES else got[side]
                    own = pltpu.roll(v_ref[side * IMAGES + img, base + q], HALF, 1)
                    first, second = (halo, own) if side == 0 else (own, halo)
                    windows[side].append((img, base + q, jnp.where(low_half, first, second)))

    def band_pass(xs, side, level):
        row = side * 2 + at_edge[side]
        coefs = [
            jnp.broadcast_to(taps_ref[row, pl.ds(level * 9 + k, 1), :], (8, LANES)) for k in range(9)
        ]
        st = 1 << level
        out = []
        for x in xs:
            acc = coefs[4] * x
            for k in (-4, -3, -2, -1, 1, 2, 3, 4):
                acc = acc + coefs[4 + k] * pltpu.roll(x, (-k * st) % LANES, 1)
            out.append(acc)
        return out

    copies = []
    for side in range(2):
        keys = [(img, k) for img, k, _ in windows[side]]
        xs = band_pass([w for _, _, w in windows[side]], side, 0)
        done = dict(zip(keys, xs))
        deeper = [key for key in keys if key[1] >= 4]
        done.update(zip(deeper, band_pass([done[key] for key in deeper], side, 1)))
        deepest = [key for key in keys if key[1] >= 6]
        done.update(zip(deepest, band_pass([done[key] for key in deepest], side, 2)))
        inside = lane < PATCH if side == 0 else lane >= LANES - PATCH
        for img in range(IMAGES):
            t = side * IMAGES + img
            for q in range(4):
                new = done[img, q]
                if q < 2:
                    new = jnp.where((lane & 1) == 0, done[img, 4 + q], new)
                if q < 1:
                    new = jnp.where((lane & 3) == 0, done[img, 6], new)
                where = (t, pl.ds(OFFSETS[q], 8, stride=4), slice(None))
                scr[where] = jnp.where(inside, pltpu.roll(new, HALF, 1), edge_in[where])
            for rt in range(4):
                copies.append(
                    _load(
                        scr.at[t, pl.ds(rt * 8, 8), :],
                        out_ref.at[img, rt, (CHUNKS - 1) * side],
                        sems.at[t, rt],
                    )
                )
    for copy in copies:
        copy.wait()


def swap(axis, even, odd):
    n = lax.axis_size(axis)
    even_pairs = [(i, i ^ 1) for i in range(n)]
    odd_pairs = [(i, i + 1 if i % 2 else i - 1) for i in range(1, n - 1)] + [(0, 0), (n - 1, n - 1)]
    via_odd = lax.ppermute(odd, axis, odd_pairs)
    via_even = lax.ppermute(even, axis, even_pairs)
    return near(via_even), near(via_odd)


def near(value):
    return pltpu.with_memory_space_constraint(value, pltpu.VMEM)


def held(*dims):
    return pltpu.VMEM(dims, F32)


VMEM = pl.BlockSpec(memory_space=pltpu.VMEM)
ANY = pl.BlockSpec(memory_space=pl.ANY)


def shape(*dims):
    return jax.ShapeDtypeStruct(dims, F32)


def transform(images):
    x = images.reshape(IMAGES, 4, 8, CHUNKS, LANES).transpose(0, 1, 3, 2, 4)
    dma = pltpu.SemaphoreType.DMA
    row_even, row_odd, block = pl.pallas_call(
        states_kernel,
        out_shape=(held(6 * TILES, LANES), held(6 * TILES, LANES), held(TILES, ROWS, LANES)),
        in_specs=[ANY],
        out_specs=(VMEM,) * 3,
        scratch_shapes=[dma((IMAGES, 4))],
        name="row_states",
    )(x)
    got_even, got_odd = swap("row", row_even, row_odd)
    rows = (near(block), near(row_even), near(row_odd), got_even, got_odd)
    v_edge, col_even, col_odd = pl.pallas_call(
        edges_kernel,
        out_shape=(held(EDGES, 7, 8, LANES), held(24, LANES), held(24, LANES)),
        in_specs=[VMEM] * 5,
        out_specs=(VMEM,) * 3,
        scratch_shapes=[pltpu.VMEM((12 * EDGES, LANES), F32)],
        name="edge_rows",
    )(*rows)
    halo_even, halo_odd = swap("col", col_even, col_odd)
    out, out_edge = pl.pallas_call(
        main_kernel,
        out_shape=(shape(IMAGES, 4, CHUNKS, 8, LANES), held(EDGES, ROWS, LANES)),
        in_specs=[VMEM] * 5,
        out_specs=(ANY, VMEM),
        scratch_shapes=[
            pltpu.VMEM((TILES, ROWS, LANES), F32),
            pltpu.VMEM((7, CHUNKS, 8, LANES), F32),
            pltpu.VMEM((12 * TILES, LANES), F32),
            dma((IMAGES, 4)),
        ],
        cost_estimate=pl.CostEstimate(flops=40_000_000, transcendentals=0, bytes_accessed=2_000_000),
        name="interior",
    )(*rows)
    out = pl.pallas_call(
        patch_kernel,
        out_shape=shape(IMAGES, 4, CHUNKS, 8, LANES),
        in_specs=[VMEM] * 5 + [ANY],
        out_specs=ANY,
        input_output_aliases={5: 0},
        scratch_shapes=[pltpu.VMEM((EDGES, ROWS, LANES), F32), dma((EDGES, 4))],
        name="edge_columns",
    )(near(jnp.asarray(EDGE_TAPS)), near(v_edge), near(out_edge), halo_even, halo_odd, out)
    return out.transpose(0, 1, 3, 2, 4).reshape(IMAGES, ROWS, CHUNKS * LANES)


def solution(mesh):
    return jax.shard_map(
        transform,
        mesh=mesh,
        in_specs=(P(None, "row", "col"),),
        out_specs=P(None, "row", "col"),
        check_vma=False,
    )
```

```python
import jax
import jax.numpy as jnp
import numpy as np
from jax import lax
from jax.experimental import pallas as pl
from jax.experimental.pallas import tpu as pltpu
from jax.sharding import PartitionSpec as P


ALPHA = -1.586134342
BETA = -0.05298011854
GAMMA = 0.8829110762
DELTA = 0.4435068522
SCALE_HIGH = 1.230174105
SCALE_LOW = 1.0 / 1.230174105

IMAGES = 4
ROWS = 32
CHUNKS = 16
TILES = IMAGES * CHUNKS
LANES = 128
EDGES = 2 * IMAGES
HALF = LANES // 2
PATCH = 32
F32 = jnp.float32
OFFSETS = (0, 2, 1, 3)
KINDS = ((0, 4, 8), (4, 2, 16), (6, 1, 32))


def tile_row(img, chunk):
    place = 0 if chunk == 0 else 1 if chunk == CHUNKS - 1 else chunk + 1
    return place * IMAGES + img


def _lift(x, left, right):
    s, d = x[0::2], x[1::2]
    m = len(s)
    d = [d[i] + ALPHA * (s[i] + (s[i + 1] if i + 1 < m else right[0])) for i in range(m)]
    s = [s[i] + BETA * ((d[i - 1] if i else left[0]) + d[i]) for i in range(m)]
    d = [d[i] + GAMMA * (s[i] + (s[i + 1] if i + 1 < m else right[1])) for i in range(m)]
    s = [s[i] + DELTA * ((d[i - 1] if i else left[1]) + d[i]) for i in range(m)]
    return [v * SCALE_LOW for v in s], [v * SCALE_HIGH for v in d]


def _states(x):
    p = x[-1] + ALPHA * x[-2]
    t = x[-2] + BETA * (x[-3] + ALPHA * (x[-4] + x[-2]))
    s = x[0]
    u = x[0] + BETA * (x[1] + ALPHA * (x[0] + x[2]))
    return p, t, s, u


def _responses():
    zero = (0.0, 0.0)
    end, start = {}, {}
    for level in (1, 2):
        for j in range(2):
            unit = (1.0, 0.0) if j == 0 else (0.0, 1.0)
            for table, left, right, pick in ((end, zero, unit, 0), (start, unit, zero, 2)):
                band = [0.0] * (ROWS >> (level - 1))
                low, _ = _lift(band, left, right)
                for into in range(level + 1, 4):
                    table[level, into, j] = _states(low)[pick : pick + 2]
                    low, _ = _lift(low, zero, zero)
    return end, start


END, START = _responses()


def _levels(x, mirror):
    out, st = [], 1
    for _ in range(3):
        s, d = list(x[0::2]), list(x[1::2])
        m = len(s)
        for odd, even in ((ALPHA, BETA), (GAMMA, DELTA)):
            for i in range(m):
                after = s[i + 1] if i + 1 < m else 0.0
                if mirror and mirror[0] == 1 and (2 * i + 2) * st > mirror[1]:
                    after = s[i]
                d[i] = d[i] + odd * (s[i] + after)
            for i in range(m):
                before = d[i - 1] if i else 0.0
                if mirror and mirror[0] == 0 and 2 * i * st == mirror[1]:
                    before = d[i]
                s[i] = s[i] + even * (before + d[i])
        s, d = [v * SCALE_LOW for v in s], [v * SCALE_HIGH for v in d]
        now = {2 * i * st: v for i, v in enumerate(s)}
        now.update({(2 * i + 1) * st: v for i, v in enumerate(d)})
        out.append(now)
        x, st = s, 2 * st
    return out


def _matrices(span, taken, given, mirror=None):
    table = np.zeros((3, taken[1], given[1]))
    for k in range(taken[1]):
        at = taken[0] + k
        if mirror and (at < mirror[1] if mirror[0] == 0 else at > mirror[1]):
            continue
        x = [0.0] * span
        x[at] = 1.0
        for level, values in enumerate(_levels(x, mirror)):
            for n in range(given[1]):
                table[level, k, n] = values.get(given[0] + n, 0.0)
    return table.astype(np.float32)


def _parts(table):
    high = table.astype(jnp.bfloat16)
    return high, (table - high.astype(np.float32)).astype(jnp.bfloat16)


def _line_matrices():
    high, low = _parts(_matrices(4 * LANES, (LANES, 2 * LANES), (LANES + HALF, LANES)))
    return np.concatenate([high, low], axis=2)


def _edge_matrices():
    out = []
    for mirror in (None, (0, 2 * LANES), (1, 2 * LANES - 1)):
        high, low = _parts(_matrices(4 * LANES, (2 * LANES - HALF, LANES), (2 * LANES - HALF, LANES), mirror))
        top = np.concatenate([high, low], axis=2)
        bottom = np.concatenate([high, np.zeros_like(high)], axis=2)
        out.append(np.concatenate([top, bottom], axis=1))
    return np.stack(out)


LINE = _line_matrices()
EDGE = _edge_matrices()


def _sub():
    return lax.broadcasted_iota(jnp.int32, (8, LANES), 0)


def _lane():
    return lax.broadcasted_iota(jnp.int32, (8, LANES), 1)


def _load(src, dst, sem):
    copy = pltpu.make_async_copy(src, dst, sem)
    copy.start()
    return copy


def _rows_of(ref, t):
    return [ref[t, pl.ds(q, 8, stride=4), :] for q in OFFSETS]


def _states_of(tile):
    sub = _sub()
    is7, is0 = sub == 7, sub == 0
    zero = jnp.zeros((8, LANES), F32)

    def up(v):
        return jnp.where(is7, zero, pltpu.roll(v, 7, 0))

    def dn(v):
        return jnp.where(is0, zero, pltpu.roll(v, 1, 0))

    a, b, c, d = tile
    c1 = c + ALPHA * (a + b)
    end = [(d + ALPHA * b)[7:8], (b + BETA * c1)[7:8]]
    start = [a[0:1], (a + BETA * c1)[0:1]]
    d1 = d + ALPHA * (b + up(a))
    a1 = a + BETA * (dn(d1) + c1)
    b1 = b + BETA * (c1 + d1)
    c2 = c1 + GAMMA * (a1 + b1)
    d2 = d1 + GAMMA * (b1 + up(a1))
    a = (a1 + DELTA * (dn(d2) + c2)) * SCALE_LOW
    b = (b1 + DELTA * (c2 + d2)) * SCALE_LOW
    b1 = b + ALPHA * (a + up(a))
    rb = dn(b1)
    end += [(b + ALPHA * a)[7:8], (a + BETA * rb)[7:8]]
    start += [a[0:1], (a + BETA * b1)[0:1]]
    a1 = a + BETA * (rb + b1)
    b2 = b1 + GAMMA * (a1 + up(a1))
    x = (a1 + DELTA * (dn(b2) + b2)) * SCALE_LOW
    back = pltpu.roll(x, 1, 0)
    x1 = x + ALPHA * (back + pltpu.roll(x, 7, 0))
    end += [(x + ALPHA * back)[7:8], (x + BETA * pltpu.roll(x1, 1, 0))[6:7]]
    start += [x[0:1], (x + BETA * pltpu.roll(x1, 7, 0))[0:1]]
    return end, start


def _junction(ends, starts):
    out = []
    for level in (1, 2, 3):
        p, t = ends[2 * level - 2], ends[2 * level - 1]
        s, u = starts[2 * level - 2], starts[2 * level - 1]
        for prior in range(1, level):
            l1, l2, r1, r2 = out[prior - 1]
            e0, e1 = END[prior, level, 0], END[prior, level, 1]
            s0, s1 = START[prior, level, 0], START[prior, level, 1]
            p = p + e0[0] * r1 + e1[0] * r2
            t = t + e0[1] * r1 + e1[1] * r2
            s = s + s0[0] * l1 + s1[0] * l2
            u = u + s0[1] * l1 + s1[1] * l2
        l1 = p + ALPHA * s
        r2 = u + BETA * l1
        l2 = l1 + GAMMA * (t + BETA * l1 + r2)
        out.append((l1, l2, s, r2))
    return out


def _boundaries(own_even, own_odd, got_even, got_odd, bnd, count):
    odd = lax.axis_index("row") % 2 == 1

    def read(ref):
        return [ref[pl.ds(k * TILES, count), :] for k in range(6)]

    oe, oo, ge, go = read(own_even), read(own_odd), read(got_even), read(got_odd)

    def pick(yes, no):
        return [jnp.where(odd, y, n) for y, n in zip(yes, no)]

    top = _junction(pick(ge, go), pick(oe, oo))
    low = _junction(pick(oo, oe), pick(go, ge))
    for level in range(3):
        for j in range(4):
            bnd[pl.ds((level * 4 + j) * count, count), :] = (top if j < 2 else low)[level][j]


def _rows_transform(tile, edge):
    row = lax.axis_index("row")
    sub = _sub()
    is7, is0 = sub == 7, sub == 0
    mir7 = is7 & (row == lax.axis_size("row") - 1)
    mir0 = is0 & (row == 0)
    odd = (sub & 1) == 1
    zero = jnp.zeros((8, LANES), F32)

    def up(v, level, j, mirror):
        return jnp.where(mir7, mirror, jnp.where(is7, edge(level, j), pltpu.roll(v, 7, 0)))

    def dn(v, level, j, mirror):
        return jnp.where(mir0, mirror, jnp.where(is0, edge(level, j), pltpu.roll(v, 1, 0)))

    a, b, c, d = tile
    c1 = c + ALPHA * (a + b)
    d1 = d + ALPHA * (b + up(a, 0, 2, b))
    a1 = a + BETA * (dn(d1, 0, 0, c1) + c1)
    b1 = b + BETA * (c1 + d1)
    c2 = c1 + GAMMA * (a1 + b1)
    d2 = d1 + GAMMA * (b1 + up(a1, 0, 3, b1))
    a = (a1 + DELTA * (dn(d2, 0, 1, c2) + c2)) * SCALE_LOW
    b = (b1 + DELTA * (c2 + d2)) * SCALE_LOW
    v = [a, b, c2 * SCALE_HIGH, d2 * SCALE_HIGH]
    b1 = b + ALPHA * (a + up(a, 1, 2, a))
    a1 = a + BETA * (dn(b1, 1, 0, b1) + b1)
    b2 = b1 + GAMMA * (a1 + up(a1, 1, 3, a1))
    x = (a1 + DELTA * (dn(b2, 1, 1, b2) + b2)) * SCALE_LOW
    v += [x, b2 * SCALE_HIGH]
    for ka, kb, j in ((ALPHA, BETA, 0), (GAMMA, DELTA, 1)):
        back = pltpu.roll(x, 1, 0)
        x = x + jnp.where(odd, ka, zero) * (back + up(x, 2, 2 + j, back))
        ahead = pltpu.roll(x, 7, 0)
        x = x + jnp.where(odd, zero, kb) * (dn(x, 2, j, ahead) + ahead)
    v.append(x * jnp.where(odd, SCALE_HIGH, zero + SCALE_LOW))
    return v


def states_kernel(x_ref, even_ref, odd_ref, scr, sems):
    copies = [
        [
            _load(
                x_ref.at[img, rt],
                scr.at[pl.ds(img * CHUNKS, CHUNKS), pl.ds(rt * 8, 8), :],
                sems.at[img, rt],
            )
            for rt in range(4)
        ]
        for img in range(IMAGES)
    ]
    is_odd = lax.axis_index("row") % 2 == 1
    for img in range(IMAGES):
        for copy in copies[img]:
            copy.wait()
        for group in range(0, CHUNKS, 4):
            got = [
                (tile_row(img, c), *_states_of(_rows_of(scr, img * CHUNKS + c))) for c in range(group, group + 4)
            ]

            def put(to_end, to_start):
                for t, end, start in got:
                    for k in range(6):
                        to_end[pl.ds(k * TILES + t, 1), :] = end[k]
                        to_start[pl.ds(k * TILES + t, 1), :] = start[k]

            pl.when(is_odd)(lambda: put(odd_ref, even_ref))
            pl.when(jnp.logical_not(is_odd))(lambda: put(even_ref, odd_ref))


def edges_kernel(x_ref, own_even, own_odd, got_even, got_odd, v_ref, even_ref, odd_ref, bnd):
    _boundaries(own_even, own_odd, got_even, got_odd, bnd, EDGES)
    lane = _lane()
    zero = jnp.zeros((8, LANES), F32)
    tiles = []
    for t in range(EDGES):

        def edge(level, j, t=t):
            return jnp.broadcast_to(bnd[pl.ds((level * 4 + j) * EDGES + t, 1), :], (8, LANES))

        column = (t % IMAGES) * CHUNKS + (t // IMAGES) * (CHUNKS - 1)
        v = _rows_transform(_rows_of(x_ref, column), edge)
        for k in range(7):
            v_ref[t, k] = v[k]
        tiles.append(v)
    is_odd = lax.axis_index("col") % 2 == 1
    for n, (base, count, width) in enumerate(KINDS):
        to_left, to_right = zero, zero
        for img in range(IMAGES):
            for q in range(count):
                slot = (img * count + q) * width
                here = (lane >= slot) & (lane < slot + width)
                start, end = tiles[img][base + q], tiles[IMAGES + img][base + q]
                if slot:
                    start = pltpu.roll(start, slot, 1)
                if (slot + width) % LANES:
                    end = pltpu.roll(end, slot + width, 1)
                to_left = jnp.where(here, start, to_left)
                to_right = jnp.where(here, end, to_right)
        even_ref[pl.ds(8 * n, 8), :] = jnp.where(is_odd, to_left, to_right)
        odd_ref[pl.ds(8 * n, 8), :] = jnp.where(is_odd, to_right, to_left)


def _split(x):
    high = x.astype(jnp.bfloat16)
    return high, (x - high.astype(F32)).astype(jnp.bfloat16)


def _dot(x, w):
    return jnp.dot(x, w, preferred_element_type=F32)


def main_kernel(w_ref, x_ref, own_even, own_odd, got_even, got_odd, out_ref, edge_ref, scr, lh1, ll1, lh2, ll2, lh3, ll3, bnd, sems):
    _boundaries(own_even, own_odd, got_even, got_odd, bnd, TILES)
    lane = _lane()
    low_half = lane < HALF
    lhs = ((lh1, ll1), (lh2, ll2), (lh3, ll3))

    def build(pair):
        before = None
        for c in range(CHUNKS + 1):
            now = before
            if c < CHUNKS:
                now = []
                for img in pair:

                    def edge(level, j, t=tile_row(img, c)):
                        return jnp.broadcast_to(bnd[pl.ds((level * 4 + j) * TILES + t, 1), :], (8, LANES))

                    v = _rows_transform(_rows_of(x_ref, img * CHUNKS + c), edge)
                    now.append([pltpu.roll(tile, HALF, 1) for tile in v])
            if before is None:
                before = now
            halves = [[jnp.where(low_half, p, q) for p, q in zip(ps, qs)] for ps, qs in zip(before, now)]
            rows1 = [tile for half in halves for tile in half[:4]]
            rows2 = [tile for half in halves for tile in half[4:6]]
            rows3 = [half[6] for half in halves]
            for (high_ref, low_ref), rows in zip(lhs, (rows1, rows2, rows3)):
                high, low = _split(jnp.concatenate(rows, axis=0))
                n = 8 * len(rows)
                for ref, part in ((high_ref, high), (low_ref, low)):
                    if c < CHUNKS:
                        ref[pl.ds(c * n, n), pl.ds(0, LANES)] = part
                    if c:
                        ref[pl.ds((c - 1) * n, n), pl.ds(LANES, LANES)] = part
            before = now

    def multiply(pair):
        outs = []
        for kind, (high_ref, low_ref) in enumerate(lhs):
            both = _dot(high_ref[...], w_ref[kind])
            outs.append(both[:, :LANES] + both[:, LANES:] + _dot(low_ref[...], w_ref[kind, :, :LANES]))
        for c in range(CHUNKS):
            for i, img in enumerate(pair):
                for q in range(4):
                    at = (c * 2 + i) * 32 + q * 8
                    val = outs[0][at : at + 8]
                    if q < 2:
                        at = (c * 2 + i) * 16 + q * 8
                        val = jnp.where((lane & 1) == 0, outs[1][at : at + 8], val)
                    if q < 1:
                        at = (c * 2 + i) * 8
                        val = jnp.where((lane & 3) == 0, outs[2][at : at + 8], val)
                    scr[img * CHUNKS + c, pl.ds(OFFSETS[q], 8, stride=4), :] = val

    stores = []
    for pair in ((0, 1), (2, 3)):
        build(pair)
        multiply(pair)
        for img in pair:
            for side, chunk in enumerate((0, CHUNKS - 1)):
                edge_ref[side * IMAGES + img] = scr[img * CHUNKS + chunk]
            for rt in range(4):
                stores.append(
                    _load(
                        scr.at[pl.ds(img * CHUNKS + 1, CHUNKS - 2), pl.ds(rt * 8, 8), :],
                        out_ref.at[img, rt, pl.ds(1, CHUNKS - 2)],
                        sems.at[img, rt],
                    )
                )
    for copy in stores:
        copy.wait()


def patch_kernel(w_ref, v_ref, edge_in, got_even, got_odd, dest_ref, out_ref, scr, sems):
    del dest_ref
    col = lax.axis_index("col")
    is_odd = col % 2 == 1
    which = (jnp.where(col == 0, 1, 0), jnp.where(col == lax.axis_size("col") - 1, 2, 0))
    lane = _lane()
    low_half = lane < HALF
    windows = [[[], [], []], [[], [], []]]
    for n, (base, count, width) in enumerate(KINDS):
        via_even, via_odd = got_even[pl.ds(8 * n, 8), :], got_odd[pl.ds(8 * n, 8), :]
        got = (jnp.where(is_odd, via_even, via_odd), jnp.where(is_odd, via_odd, via_even))
        for img in range(IMAGES):
            for q in range(count):
                slot = (img * count + q) * width
                for side, shift in ((0, HALF - slot - width), (1, HALF - slot)):
                    halo = pltpu.roll(got[side], shift % LANES, 1) if shift % LANES else got[side]
                    own = pltpu.roll(v_ref[side * IMAGES + img, base + q], HALF, 1)
                    first, second = (halo, own) if side == 0 else (own, halo)
                    windows[side][n].append(jnp.where(low_half, first, second))
    copies = []
    for side in range(2):
        outs = []
        for n in range(3):
            x = jnp.concatenate(windows[side][n], axis=0)
            y = _dot(jnp.concatenate(_split(x), axis=1), w_ref[which[side], n])
            outs.append(y[:, :LANES] + y[:, LANES:])
        inside = lane < PATCH if side == 0 else lane >= LANES - PATCH
        for img in range(IMAGES):
            t = side * IMAGES + img
            for q in range(4):
                at = (img * 4 + q) * 8
                new = outs[0][at : at + 8]
                if q < 2:
                    at = (img * 2 + q) * 8
                    new = jnp.where((lane & 1) == 0, outs[1][at : at + 8], new)
                if q < 1:
                    new = jnp.where((lane & 3) == 0, outs[2][img * 8 : img * 8 + 8], new)
                where = (t, pl.ds(OFFSETS[q], 8, stride=4), slice(None))
                scr[where] = jnp.where(inside, pltpu.roll(new, HALF, 1), edge_in[where])
            for rt in range(4):
                copies.append(
                    _load(
                        scr.at[t, pl.ds(rt * 8, 8), :],
                        out_ref.at[img, rt, (CHUNKS - 1) * side],
                        sems.at[t, rt],
                    )
                )
    for copy in copies:
        copy.wait()


def swap(axis, even, odd):
    n = lax.axis_size(axis)
    even_pairs = [(i, i ^ 1) for i in range(n)]
    odd_pairs = [(i, i + 1 if i % 2 else i - 1) for i in range(1, n - 1)] + [(0, 0), (n - 1, n - 1)]
    via_odd = lax.ppermute(odd, axis, odd_pairs)
    via_even = lax.ppermute(even, axis, even_pairs)
    return near(via_even), near(via_odd)


def near(value):
    return pltpu.with_memory_space_constraint(value, pltpu.VMEM)


def held(*dims):
    return pltpu.VMEM(dims, F32)


VMEM = pl.BlockSpec(memory_space=pltpu.VMEM)
ANY = pl.BlockSpec(memory_space=pl.ANY)


def shape(*dims):
    return jax.ShapeDtypeStruct(dims, F32)


def transform(images):
    x = images.reshape(IMAGES, 4, 8, CHUNKS, LANES).transpose(0, 1, 3, 2, 4)
    dma = pltpu.SemaphoreType.DMA
    row_even, row_odd, block = pl.pallas_call(
        states_kernel,
        out_shape=(held(6 * TILES, LANES), held(6 * TILES, LANES), held(TILES, ROWS, LANES)),
        in_specs=[ANY],
        out_specs=(VMEM,) * 3,
        scratch_shapes=[dma((IMAGES, 4))],
        name="row_states",
    )(x)
    got_even, got_odd = swap("row", row_even, row_odd)
    rows = (near(block), near(row_even), near(row_odd), got_even, got_odd)
    v_edge, col_even, col_odd = pl.pallas_call(
        edges_kernel,
        out_shape=(held(EDGES, 7, 8, LANES), held(24, LANES), held(24, LANES)),
        in_specs=[VMEM] * 5,
        out_specs=(VMEM,) * 3,
        scratch_shapes=[pltpu.VMEM((12 * EDGES, LANES), F32)],
        name="edge_rows",
    )(*rows)
    halo_even, halo_odd = swap("col", col_even, col_odd)
    out, out_edge = pl.pallas_call(
        main_kernel,
        out_shape=(shape(IMAGES, 4, CHUNKS, 8, LANES), held(EDGES, ROWS, LANES)),
        in_specs=[VMEM] * 6,
        out_specs=(ANY, VMEM),
        scratch_shapes=[
            pltpu.VMEM((TILES, ROWS, LANES), F32),
            *(pltpu.VMEM((CHUNKS * n, 2 * LANES), jnp.bfloat16) for n in (64, 64, 32, 32, 16, 16)),
            pltpu.VMEM((12 * TILES, LANES), F32),
            dma((IMAGES, 4)),
        ],
        cost_estimate=pl.CostEstimate(flops=40_000_000, transcendentals=0, bytes_accessed=2_000_000),
        name="interior",
    )(near(jnp.asarray(LINE)), *rows)
    out = pl.pallas_call(
        patch_kernel,
        out_shape=shape(IMAGES, 4, CHUNKS, 8, LANES),
        in_specs=[VMEM] * 5 + [ANY],
        out_specs=ANY,
        input_output_aliases={5: 0},
        scratch_shapes=[pltpu.VMEM((EDGES, ROWS, LANES), F32), dma((EDGES, 4))],
        name="edge_columns",
    )(near(jnp.asarray(EDGE)), near(v_edge), near(out_edge), halo_even, halo_odd, out)
    return out.transpose(0, 1, 3, 2, 4).reshape(IMAGES, ROWS, CHUNKS * LANES)


def solution(mesh):
    return jax.shard_map(
        transform,
        mesh=mesh,
        in_specs=(P(None, "row", "col"),),
        out_specs=P(None, "row", "col"),
        check_vma=False,
    )
```

```python
import jax
import jax.numpy as jnp
import numpy as np
from jax import lax
from jax.experimental import pallas as pl
from jax.experimental.pallas import tpu as pltpu
from jax.sharding import PartitionSpec as P


ALPHA = -1.586134342
BETA = -0.05298011854
GAMMA = 0.8829110762
DELTA = 0.4435068522
SCALE_HIGH = 1.230174105
SCALE_LOW = 1.0 / 1.230174105

IMAGES = 4
ROWS = 32
CHUNKS = 16
TILES = IMAGES * CHUNKS
LANES = 128
EDGES = 2 * IMAGES
HALF = LANES // 2
PATCH = 32
F32 = jnp.float32
OFFSETS = (0, 2, 1, 3)
KINDS = ((0, 4, 8), (4, 2, 16), (6, 1, 32))


def tile_row(img, chunk):
    place = 0 if chunk == 0 else 1 if chunk == CHUNKS - 1 else chunk + 1
    return place * IMAGES + img


def _lift(x, left, right):
    s, d = x[0::2], x[1::2]
    m = len(s)
    d = [d[i] + ALPHA * (s[i] + (s[i + 1] if i + 1 < m else right[0])) for i in range(m)]
    s = [s[i] + BETA * ((d[i - 1] if i else left[0]) + d[i]) for i in range(m)]
    d = [d[i] + GAMMA * (s[i] + (s[i + 1] if i + 1 < m else right[1])) for i in range(m)]
    s = [s[i] + DELTA * ((d[i - 1] if i else left[1]) + d[i]) for i in range(m)]
    return [v * SCALE_LOW for v in s], [v * SCALE_HIGH for v in d]


def _states(x):
    p = x[-1] + ALPHA * x[-2]
    t = x[-2] + BETA * (x[-3] + ALPHA * (x[-4] + x[-2]))
    s = x[0]
    u = x[0] + BETA * (x[1] + ALPHA * (x[0] + x[2]))
    return p, t, s, u


def _responses():
    zero = (0.0, 0.0)
    end, start = {}, {}
    for level in (1, 2):
        for j in range(2):
            unit = (1.0, 0.0) if j == 0 else (0.0, 1.0)
            for table, left, right, pick in ((end, zero, unit, 0), (start, unit, zero, 2)):
                band = [0.0] * (ROWS >> (level - 1))
                low, _ = _lift(band, left, right)
                for into in range(level + 1, 4):
                    table[level, into, j] = _states(low)[pick : pick + 2]
                    low, _ = _lift(low, zero, zero)
    return end, start


END, START = _responses()


def _levels(x, mirror):
    out, st = [], 1
    for _ in range(3):
        s, d = list(x[0::2]), list(x[1::2])
        m = len(s)
        for odd, even in ((ALPHA, BETA), (GAMMA, DELTA)):
            for i in range(m):
                after = s[i + 1] if i + 1 < m else 0.0
                if mirror and mirror[0] == 1 and (2 * i + 2) * st > mirror[1]:
                    after = s[i]
                d[i] = d[i] + odd * (s[i] + after)
            for i in range(m):
                before = d[i - 1] if i else 0.0
                if mirror and mirror[0] == 0 and 2 * i * st == mirror[1]:
                    before = d[i]
                s[i] = s[i] + even * (before + d[i])
        s, d = [v * SCALE_LOW for v in s], [v * SCALE_HIGH for v in d]
        now = {2 * i * st: v for i, v in enumerate(s)}
        now.update({(2 * i + 1) * st: v for i, v in enumerate(d)})
        out.append(now)
        x, st = s, 2 * st
    return out


def _matrices(span, taken, given, mirror=None):
    table = np.zeros((3, taken[1], given[1]))
    for k in range(taken[1]):
        at = taken[0] + k
        if mirror and (at < mirror[1] if mirror[0] == 0 else at > mirror[1]):
            continue
        x = [0.0] * span
        x[at] = 1.0
        for level, values in enumerate(_levels(x, mirror)):
            for n in range(given[1]):
                table[level, k, n] = values.get(given[0] + n, 0.0)
    return table.astype(np.float32)


def _parts(table):
    high = table.astype(jnp.bfloat16)
    return high, (table - high.astype(np.float32)).astype(jnp.bfloat16)


def _line_matrices():
    high, low = _parts(_matrices(4 * LANES, (LANES, 2 * LANES), (LANES + HALF, LANES)))
    return np.concatenate([high, low], axis=2)


def _edge_matrices():
    out = []
    for mirror in (None, (0, 2 * LANES), (1, 2 * LANES - 1)):
        high, low = _parts(_matrices(4 * LANES, (2 * LANES - HALF, LANES), (2 * LANES - HALF, LANES), mirror))
        top = np.concatenate([high, low], axis=2)
        bottom = np.concatenate([high, np.zeros_like(high)], axis=2)
        out.append(np.concatenate([top, bottom], axis=1))
    return np.stack(out)


LINE = _line_matrices()
EDGE = _edge_matrices()


def _sub():
    return lax.broadcasted_iota(jnp.int32, (8, LANES), 0)


def _lane():
    return lax.broadcasted_iota(jnp.int32, (8, LANES), 1)


def _load(src, dst, sem):
    copy = pltpu.make_async_copy(src, dst, sem)
    copy.start()
    return copy


def _rows_of(ref, t):
    return [ref[t, pl.ds(q, 8, stride=4), :] for q in OFFSETS]


def _states_of(tile):
    sub = _sub()
    is7, is0 = sub == 7, sub == 0
    zero = jnp.zeros((8, LANES), F32)

    def up(v):
        return jnp.where(is7, zero, pltpu.roll(v, 7, 0))

    def dn(v):
        return jnp.where(is0, zero, pltpu.roll(v, 1, 0))

    a, b, c, d = tile
    c1 = c + ALPHA * (a + b)
    end = [(d + ALPHA * b)[7:8], (b + BETA * c1)[7:8]]
    start = [a[0:1], (a + BETA * c1)[0:1]]
    d1 = d + ALPHA * (b + up(a))
    a1 = a + BETA * (dn(d1) + c1)
    b1 = b + BETA * (c1 + d1)
    c2 = c1 + GAMMA * (a1 + b1)
    d2 = d1 + GAMMA * (b1 + up(a1))
    a = (a1 + DELTA * (dn(d2) + c2)) * SCALE_LOW
    b = (b1 + DELTA * (c2 + d2)) * SCALE_LOW
    b1 = b + ALPHA * (a + up(a))
    rb = dn(b1)
    end += [(b + ALPHA * a)[7:8], (a + BETA * rb)[7:8]]
    start += [a[0:1], (a + BETA * b1)[0:1]]
    a1 = a + BETA * (rb + b1)
    b2 = b1 + GAMMA * (a1 + up(a1))
    x = (a1 + DELTA * (dn(b2) + b2)) * SCALE_LOW
    back = pltpu.roll(x, 1, 0)
    x1 = x + ALPHA * (back + pltpu.roll(x, 7, 0))
    end += [(x + ALPHA * back)[7:8], (x + BETA * pltpu.roll(x1, 1, 0))[6:7]]
    start += [x[0:1], (x + BETA * pltpu.roll(x1, 7, 0))[0:1]]
    return end, start


def _junction(ends, starts):
    out = []
    for level in (1, 2, 3):
        p, t = ends[2 * level - 2], ends[2 * level - 1]
        s, u = starts[2 * level - 2], starts[2 * level - 1]
        for prior in range(1, level):
            l1, l2, r1, r2 = out[prior - 1]
            e0, e1 = END[prior, level, 0], END[prior, level, 1]
            s0, s1 = START[prior, level, 0], START[prior, level, 1]
            p = p + e0[0] * r1 + e1[0] * r2
            t = t + e0[1] * r1 + e1[1] * r2
            s = s + s0[0] * l1 + s1[0] * l2
            u = u + s0[1] * l1 + s1[1] * l2
        l1 = p + ALPHA * s
        r2 = u + BETA * l1
        l2 = l1 + GAMMA * (t + BETA * l1 + r2)
        out.append((l1, l2, s, r2))
    return out


def _boundaries(own_even, own_odd, got_even, got_odd, bnd, count):
    odd = lax.axis_index("row") % 2 == 1

    def read(ref):
        return [ref[pl.ds(k * TILES, count), :] for k in range(6)]

    oe, oo, ge, go = read(own_even), read(own_odd), read(got_even), read(got_odd)

    def pick(yes, no):
        return [jnp.where(odd, y, n) for y, n in zip(yes, no)]

    top = _junction(pick(ge, go), pick(oe, oo))
    low = _junction(pick(oo, oe), pick(go, ge))
    for level in range(3):
        for j in range(4):
            bnd[pl.ds((level * 4 + j) * count, count), :] = (top if j < 2 else low)[level][j]


def _rows_transform(tile, edge):
    row = lax.axis_index("row")
    sub = _sub()
    is7, is0 = sub == 7, sub == 0
    mir7 = is7 & (row == lax.axis_size("row") - 1)
    mir0 = is0 & (row == 0)
    odd = (sub & 1) == 1
    zero = jnp.zeros((8, LANES), F32)

    def up(v, level, j, mirror):
        return jnp.where(mir7, mirror, jnp.where(is7, edge(level, j), pltpu.roll(v, 7, 0)))

    def dn(v, level, j, mirror):
        return jnp.where(mir0, mirror, jnp.where(is0, edge(level, j), pltpu.roll(v, 1, 0)))

    a, b, c, d = tile
    c1 = c + ALPHA * (a + b)
    d1 = d + ALPHA * (b + up(a, 0, 2, b))
    a1 = a + BETA * (dn(d1, 0, 0, c1) + c1)
    b1 = b + BETA * (c1 + d1)
    c2 = c1 + GAMMA * (a1 + b1)
    d2 = d1 + GAMMA * (b1 + up(a1, 0, 3, b1))
    a = (a1 + DELTA * (dn(d2, 0, 1, c2) + c2)) * SCALE_LOW
    b = (b1 + DELTA * (c2 + d2)) * SCALE_LOW
    v = [a, b, c2 * SCALE_HIGH, d2 * SCALE_HIGH]
    b1 = b + ALPHA * (a + up(a, 1, 2, a))
    a1 = a + BETA * (dn(b1, 1, 0, b1) + b1)
    b2 = b1 + GAMMA * (a1 + up(a1, 1, 3, a1))
    x = (a1 + DELTA * (dn(b2, 1, 1, b2) + b2)) * SCALE_LOW
    v += [x, b2 * SCALE_HIGH]
    for ka, kb, j in ((ALPHA, BETA, 0), (GAMMA, DELTA, 1)):
        back = pltpu.roll(x, 1, 0)
        x = x + jnp.where(odd, ka, zero) * (back + up(x, 2, 2 + j, back))
        ahead = pltpu.roll(x, 7, 0)
        x = x + jnp.where(odd, zero, kb) * (dn(x, 2, j, ahead) + ahead)
    v.append(x * jnp.where(odd, SCALE_HIGH, zero + SCALE_LOW))
    return v


def states_kernel(x_ref, even_ref, odd_ref, scr, sems):
    copies = [
        [
            _load(
                x_ref.at[img, rt],
                scr.at[pl.ds(img * CHUNKS, CHUNKS), pl.ds(rt * 8, 8), :],
                sems.at[img, rt],
            )
            for rt in range(4)
        ]
        for img in range(IMAGES)
    ]
    is_odd = lax.axis_index("row") % 2 == 1
    for img in range(IMAGES):
        for copy in copies[img]:
            copy.wait()
        for group in range(0, CHUNKS, 4):
            got = [
                (tile_row(img, c), *_states_of(_rows_of(scr, img * CHUNKS + c))) for c in range(group, group + 4)
            ]

            def put(to_end, to_start):
                for t, end, start in got:
                    for k in range(6):
                        to_end[pl.ds(k * TILES + t, 1), :] = end[k]
                        to_start[pl.ds(k * TILES + t, 1), :] = start[k]

            pl.when(is_odd)(lambda: put(odd_ref, even_ref))
            pl.when(jnp.logical_not(is_odd))(lambda: put(even_ref, odd_ref))


def edges_kernel(x_ref, own_even, own_odd, got_even, got_odd, v_ref, even_ref, odd_ref, bnd):
    _boundaries(own_even, own_odd, got_even, got_odd, bnd, EDGES)
    lane = _lane()
    zero = jnp.zeros((8, LANES), F32)
    tiles = []
    for t in range(EDGES):

        def edge(level, j, t=t):
            return jnp.broadcast_to(bnd[pl.ds((level * 4 + j) * EDGES + t, 1), :], (8, LANES))

        column = (t % IMAGES) * CHUNKS + (t // IMAGES) * (CHUNKS - 1)
        v = _rows_transform(_rows_of(x_ref, column), edge)
        for k in range(7):
            v_ref[t, k] = v[k]
        tiles.append(v)
    is_odd = lax.axis_index("col") % 2 == 1
    for n, (base, count, width) in enumerate(KINDS):
        to_left, to_right = zero, zero
        for img in range(IMAGES):
            for q in range(count):
                slot = (img * count + q) * width
                here = (lane >= slot) & (lane < slot + width)
                start, end = tiles[img][base + q], tiles[IMAGES + img][base + q]
                if slot:
                    start = pltpu.roll(start, slot, 1)
                if (slot + width) % LANES:
                    end = pltpu.roll(end, slot + width, 1)
                to_left = jnp.where(here, start, to_left)
                to_right = jnp.where(here, end, to_right)
        even_ref[pl.ds(8 * n, 8), :] = jnp.where(is_odd, to_left, to_right)
        odd_ref[pl.ds(8 * n, 8), :] = jnp.where(is_odd, to_right, to_left)


def _split(x):
    high = x.astype(jnp.bfloat16)
    return high, (x - high.astype(F32)).astype(jnp.bfloat16)


def _dot(x, w):
    return jnp.dot(x, w, preferred_element_type=F32)


def main_kernel(later_ref, w_ref, x_ref, own_even, own_odd, got_even, got_odd, out_ref, edge_ref, scr, lh1, ll1, lh2, ll2, lh3, ll3, bnd, sems):
    del later_ref
    _boundaries(own_even, own_odd, got_even, got_odd, bnd, TILES)
    lane = _lane()
    low_half = lane < HALF
    lhs = ((lh1, ll1), (lh2, ll2), (lh3, ll3))

    def build(pair):
        before = None
        for c in range(CHUNKS + 1):
            now = before
            if c < CHUNKS:
                now = []
                for img in pair:

                    def edge(level, j, t=tile_row(img, c)):
                        return jnp.broadcast_to(bnd[pl.ds((level * 4 + j) * TILES + t, 1), :], (8, LANES))

                    v = _rows_transform(_rows_of(x_ref, img * CHUNKS + c), edge)
                    now.append([pltpu.roll(tile, HALF, 1) for tile in v])
            if before is None:
                before = now
            halves = [[jnp.where(low_half, p, q) for p, q in zip(ps, qs)] for ps, qs in zip(before, now)]
            rows1 = [tile for half in halves for tile in half[:4]]
            rows2 = [tile for half in halves for tile in half[4:6]]
            rows3 = [half[6] for half in halves]
            for (high_ref, low_ref), rows in zip(lhs, (rows1, rows2, rows3)):
                high, low = _split(jnp.concatenate(rows, axis=0))
                n = 8 * len(rows)
                for ref, part in ((high_ref, high), (low_ref, low)):
                    if c < CHUNKS:
                        ref[pl.ds(c * n, n), pl.ds(0, LANES)] = part
                    if c:
                        ref[pl.ds((c - 1) * n, n), pl.ds(LANES, LANES)] = part
            before = now

    def multiply(pair):
        outs = []
        for kind, (high_ref, low_ref) in enumerate(lhs):
            both = _dot(high_ref[...], w_ref[kind])
            outs.append(both[:, :LANES] + both[:, LANES:] + _dot(low_ref[...], w_ref[kind, :, :LANES]))
        for c in range(CHUNKS):
            for i, img in enumerate(pair):
                for q in range(4):
                    at = (c * 2 + i) * 32 + q * 8
                    val = outs[0][at : at + 8]
                    if q < 2:
                        at = (c * 2 + i) * 16 + q * 8
                        val = jnp.where((lane & 1) == 0, outs[1][at : at + 8], val)
                    if q < 1:
                        at = (c * 2 + i) * 8
                        val = jnp.where((lane & 3) == 0, outs[2][at : at + 8], val)
                    scr[img * CHUNKS + c, pl.ds(OFFSETS[q], 8, stride=4), :] = val

    stores = []
    for pair in ((0, 1), (2, 3)):
        build(pair)
        multiply(pair)
        for img in pair:
            for side, chunk in enumerate((0, CHUNKS - 1)):
                edge_ref[side * IMAGES + img] = scr[img * CHUNKS + chunk]
            for rt in range(4):
                stores.append(
                    _load(
                        scr.at[pl.ds(img * CHUNKS + 1, CHUNKS - 2), pl.ds(rt * 8, 8), :],
                        out_ref.at[img, rt, pl.ds(1, CHUNKS - 2)],
                        sems.at[img, rt],
                    )
                )
    for copy in stores:
        copy.wait()


def patch_kernel(w_ref, v_ref, edge_in, got_even, got_odd, dest_ref, out_ref, scr, sems):
    del dest_ref
    col = lax.axis_index("col")
    is_odd = col % 2 == 1
    which = (jnp.where(col == 0, 1, 0), jnp.where(col == lax.axis_size("col") - 1, 2, 0))
    lane = _lane()
    low_half = lane < HALF
    windows = [[[], [], []], [[], [], []]]
    for n, (base, count, width) in enumerate(KINDS):
        via_even, via_odd = got_even[pl.ds(8 * n, 8), :], got_odd[pl.ds(8 * n, 8), :]
        got = (jnp.where(is_odd, via_even, via_odd), jnp.where(is_odd, via_odd, via_even))
        for img in range(IMAGES):
            for q in range(count):
                slot = (img * count + q) * width
                for side, shift in ((0, HALF - slot - width), (1, HALF - slot)):
                    halo = pltpu.roll(got[side], shift % LANES, 1) if shift % LANES else got[side]
                    own = pltpu.roll(v_ref[side * IMAGES + img, base + q], HALF, 1)
                    first, second = (halo, own) if side == 0 else (own, halo)
                    windows[side][n].append(jnp.where(low_half, first, second))
    copies = []
    for side in range(2):
        outs = []
        for n in range(3):
            x = jnp.concatenate(windows[side][n], axis=0)
            y = _dot(jnp.concatenate(_split(x), axis=1), w_ref[which[side], n])
            outs.append(y[:, :LANES] + y[:, LANES:])
        inside = lane < PATCH if side == 0 else lane >= LANES - PATCH
        for img in range(IMAGES):
            t = side * IMAGES + img
            for q in range(4):
                at = (img * 4 + q) * 8
                new = outs[0][at : at + 8]
                if q < 2:
                    at = (img * 2 + q) * 8
                    new = jnp.where((lane & 1) == 0, outs[1][at : at + 8], new)
                if q < 1:
                    new = jnp.where((lane & 3) == 0, outs[2][img * 8 : img * 8 + 8], new)
                where = (t, pl.ds(OFFSETS[q], 8, stride=4), slice(None))
                scr[where] = jnp.where(inside, pltpu.roll(new, HALF, 1), edge_in[where])
            column = scr.reshape(EDGES, 4, 8, LANES).at[t]
            copies.append(_load(column, out_ref.at[img, :, (CHUNKS - 1) * side], sems.at[t]))
    for copy in copies:
        copy.wait()


def swap(axis, even, odd):
    n = lax.axis_size(axis)
    even_pairs = [(i, i ^ 1) for i in range(n)]
    odd_pairs = [(i, i + 1 if i % 2 else i - 1) for i in range(1, n - 1)] + [(0, 0), (n - 1, n - 1)]
    via_odd = lax.ppermute(odd, axis, odd_pairs)
    via_even = lax.ppermute(even, axis, even_pairs)
    return near(via_even), near(via_odd)


def near(value):
    return pltpu.with_memory_space_constraint(value, pltpu.VMEM)


def held(*dims):
    return pltpu.VMEM(dims, F32)


VMEM = pl.BlockSpec(memory_space=pltpu.VMEM)
ANY = pl.BlockSpec(memory_space=pl.ANY)


def shape(*dims):
    return jax.ShapeDtypeStruct(dims, F32)


def transform(images):
    x = images.reshape(IMAGES, 4, 8, CHUNKS, LANES).transpose(0, 1, 3, 2, 4)
    dma = pltpu.SemaphoreType.DMA
    row_even, row_odd, block = pl.pallas_call(
        states_kernel,
        out_shape=(held(6 * TILES, LANES), held(6 * TILES, LANES), held(TILES, ROWS, LANES)),
        in_specs=[ANY],
        out_specs=(VMEM,) * 3,
        scratch_shapes=[dma((IMAGES, 4))],
        compiler_params=pltpu.CompilerParams(vmem_limit_bytes=8 << 20),
        name="row_states",
    )(pltpu.with_memory_space_constraint(x, pltpu.HBM))
    got_even, got_odd = swap("row", row_even, row_odd)
    rows = (near(block), near(row_even), near(row_odd), got_even, got_odd)
    v_edge, col_even, col_odd = pl.pallas_call(
        edges_kernel,
        out_shape=(held(EDGES, 7, 8, LANES), held(24, LANES), held(24, LANES)),
        in_specs=[VMEM] * 5,
        out_specs=(VMEM,) * 3,
        scratch_shapes=[pltpu.VMEM((12 * EDGES, LANES), F32)],
        compiler_params=pltpu.CompilerParams(vmem_limit_bytes=8 << 20),
        name="edge_rows",
    )(*rows)
    edge_matrices = near(jnp.asarray(EDGE))
    halo_even, halo_odd = swap("col", col_even, col_odd)
    out, out_edge = pl.pallas_call(
        main_kernel,
        out_shape=(shape(IMAGES, 4, CHUNKS, 8, LANES), held(EDGES, ROWS, LANES)),
        in_specs=[VMEM] * 7,
        out_specs=(ANY, VMEM),
        scratch_shapes=[
            pltpu.VMEM((TILES, ROWS, LANES), F32),
            *(pltpu.VMEM((CHUNKS * n, 2 * LANES), jnp.bfloat16) for n in (64, 64, 32, 32, 16, 16)),
            pltpu.VMEM((12 * TILES, LANES), F32),
            dma((IMAGES, 4)),
        ],
        cost_estimate=pl.CostEstimate(flops=40_000_000, transcendentals=0, bytes_accessed=2_000_000),
        compiler_params=pltpu.CompilerParams(vmem_limit_bytes=24 << 20),
        name="interior",
    )(edge_matrices, near(jnp.asarray(LINE)), *rows)
    out = pl.pallas_call(
        patch_kernel,
        out_shape=shape(IMAGES, 4, CHUNKS, 8, LANES),
        in_specs=[VMEM] * 5 + [ANY],
        out_specs=ANY,
        input_output_aliases={5: 0},
        scratch_shapes=[pltpu.VMEM((EDGES, ROWS, LANES), F32), dma((EDGES,))],
        compiler_params=pltpu.CompilerParams(vmem_limit_bytes=8 << 20),
        name="edge_columns",
    )(edge_matrices, near(v_edge), near(out_edge), halo_even, halo_odd, out)
    return out.transpose(0, 1, 3, 2, 4).reshape(IMAGES, ROWS, CHUNKS * LANES)


def solution(mesh):
    return jax.shard_map(
        transform,
        mesh=mesh,
        in_specs=(P(None, "row", "col"),),
        out_specs=P(None, "row", "col"),
        check_vma=False,
    )
```

```python
import jax
import jax.numpy as jnp
import numpy as np
from jax import lax
from jax.experimental import pallas as pl
from jax.experimental.pallas import tpu as pltpu
from jax.sharding import PartitionSpec as P


ALPHA = -1.586134342
BETA = -0.05298011854
GAMMA = 0.8829110762
DELTA = 0.4435068522
SCALE_HIGH = 1.230174105
SCALE_LOW = 1.0 / 1.230174105

IMAGES = 4
ROWS = 32
CHUNKS = 16
TILES = IMAGES * CHUNKS
LANES = 128
EDGES = 2 * IMAGES
HALF = LANES // 2
PATCH = 32
F32 = jnp.float32
OFFSETS = (0, 2, 1, 3)
KINDS = ((0, 4, 8), (4, 2, 16), (6, 1, 32))


def tile_row(img, chunk):
    place = 0 if chunk == 0 else 1 if chunk == CHUNKS - 1 else chunk + 1
    return place * IMAGES + img


def _lift(x, left, right):
    s, d = x[0::2], x[1::2]
    m = len(s)
    d = [d[i] + ALPHA * (s[i] + (s[i + 1] if i + 1 < m else right[0])) for i in range(m)]
    s = [s[i] + BETA * ((d[i - 1] if i else left[0]) + d[i]) for i in range(m)]
    d = [d[i] + GAMMA * (s[i] + (s[i + 1] if i + 1 < m else right[1])) for i in range(m)]
    s = [s[i] + DELTA * ((d[i - 1] if i else left[1]) + d[i]) for i in range(m)]
    return [v * SCALE_LOW for v in s], [v * SCALE_HIGH for v in d]


def _states(x):
    p = x[-1] + ALPHA * x[-2]
    t = x[-2] + BETA * (x[-3] + ALPHA * (x[-4] + x[-2]))
    s = x[0]
    u = x[0] + BETA * (x[1] + ALPHA * (x[0] + x[2]))
    return p, t, s, u


def _responses():
    zero = (0.0, 0.0)
    end, start = {}, {}
    for level in (1, 2):
        for j in range(2):
            unit = (1.0, 0.0) if j == 0 else (0.0, 1.0)
            for table, left, right, pick in ((end, zero, unit, 0), (start, unit, zero, 2)):
                band = [0.0] * (ROWS >> (level - 1))
                low, _ = _lift(band, left, right)
                for into in range(level + 1, 4):
                    table[level, into, j] = _states(low)[pick : pick + 2]
                    low, _ = _lift(low, zero, zero)
    return end, start


END, START = _responses()


def _levels(x, mirror):
    out, st = [], 1
    for _ in range(3):
        s, d = list(x[0::2]), list(x[1::2])
        m = len(s)
        for odd, even in ((ALPHA, BETA), (GAMMA, DELTA)):
            for i in range(m):
                after = s[i + 1] if i + 1 < m else 0.0
                if mirror and mirror[0] == 1 and (2 * i + 2) * st > mirror[1]:
                    after = s[i]
                d[i] = d[i] + odd * (s[i] + after)
            for i in range(m):
                before = d[i - 1] if i else 0.0
                if mirror and mirror[0] == 0 and 2 * i * st == mirror[1]:
                    before = d[i]
                s[i] = s[i] + even * (before + d[i])
        s, d = [v * SCALE_LOW for v in s], [v * SCALE_HIGH for v in d]
        now = {2 * i * st: v for i, v in enumerate(s)}
        now.update({(2 * i + 1) * st: v for i, v in enumerate(d)})
        out.append(now)
        x, st = s, 2 * st
    return out


def _matrices(span, taken, given, mirror=None):
    table = np.zeros((3, taken[1], given[1]))
    for k in range(taken[1]):
        at = taken[0] + k
        if mirror and (at < mirror[1] if mirror[0] == 0 else at > mirror[1]):
            continue
        x = [0.0] * span
        x[at] = 1.0
        for level, values in enumerate(_levels(x, mirror)):
            for n in range(given[1]):
                table[level, k, n] = values.get(given[0] + n, 0.0)
    return table.astype(np.float32)


def _parts(table):
    high = table.astype(jnp.bfloat16)
    return high, (table - high.astype(np.float32)).astype(jnp.bfloat16)


def _line_matrices():
    high, low = _parts(_matrices(4 * LANES, (LANES, 2 * LANES), (LANES + HALF, LANES)))
    return np.concatenate([high, low], axis=2)


def _edge_matrices():
    out = []
    for mirror in (None, (0, 2 * LANES), (1, 2 * LANES - 1)):
        high, low = _parts(_matrices(4 * LANES, (2 * LANES - HALF, LANES), (2 * LANES - HALF, LANES), mirror))
        top = np.concatenate([high, low], axis=2)
        bottom = np.concatenate([high, np.zeros_like(high)], axis=2)
        out.append(np.concatenate([top, bottom], axis=1))
    return np.stack(out)


LINE = _line_matrices()
EDGE = _edge_matrices()


def _sub():
    return lax.broadcasted_iota(jnp.int32, (8, LANES), 0)


def _lane():
    return lax.broadcasted_iota(jnp.int32, (8, LANES), 1)


def _load(src, dst, sem):
    copy = pltpu.make_async_copy(src, dst, sem)
    copy.start()
    return copy


def _rows_of(ref, t):
    return [ref[t, pl.ds(q, 8, stride=4), :] for q in OFFSETS]


def _states_of(tile):
    sub = _sub()
    is7, is0 = sub == 7, sub == 0
    zero = jnp.zeros((8, LANES), F32)

    def up(v):
        return jnp.where(is7, zero, pltpu.roll(v, 7, 0))

    def dn(v):
        return jnp.where(is0, zero, pltpu.roll(v, 1, 0))

    a, b, c, d = tile
    c1 = c + ALPHA * (a + b)
    end = [(d + ALPHA * b)[7:8], (b + BETA * c1)[7:8]]
    start = [a[0:1], (a + BETA * c1)[0:1]]
    d1 = d + ALPHA * (b + up(a))
    a1 = a + BETA * (dn(d1) + c1)
    b1 = b + BETA * (c1 + d1)
    c2 = c1 + GAMMA * (a1 + b1)
    d2 = d1 + GAMMA * (b1 + up(a1))
    a = (a1 + DELTA * (dn(d2) + c2)) * SCALE_LOW
    b = (b1 + DELTA * (c2 + d2)) * SCALE_LOW
    b1 = b + ALPHA * (a + up(a))
    rb = dn(b1)
    end += [(b + ALPHA * a)[7:8], (a + BETA * rb)[7:8]]
    start += [a[0:1], (a + BETA * b1)[0:1]]
    a1 = a + BETA * (rb + b1)
    b2 = b1 + GAMMA * (a1 + up(a1))
    x = (a1 + DELTA * (dn(b2) + b2)) * SCALE_LOW
    back = pltpu.roll(x, 1, 0)
    x1 = x + ALPHA * (back + pltpu.roll(x, 7, 0))
    end += [(x + ALPHA * back)[7:8], (x + BETA * pltpu.roll(x1, 1, 0))[6:7]]
    start += [x[0:1], (x + BETA * pltpu.roll(x1, 7, 0))[0:1]]
    return end, start


def _junction(ends, starts):
    out = []
    for level in (1, 2, 3):
        p, t = ends[2 * level - 2], ends[2 * level - 1]
        s, u = starts[2 * level - 2], starts[2 * level - 1]
        for prior in range(1, level):
            l1, l2, r1, r2 = out[prior - 1]
            e0, e1 = END[prior, level, 0], END[prior, level, 1]
            s0, s1 = START[prior, level, 0], START[prior, level, 1]
            p = p + e0[0] * r1 + e1[0] * r2
            t = t + e0[1] * r1 + e1[1] * r2
            s = s + s0[0] * l1 + s1[0] * l2
            u = u + s0[1] * l1 + s1[1] * l2
        l1 = p + ALPHA * s
        r2 = u + BETA * l1
        l2 = l1 + GAMMA * (t + BETA * l1 + r2)
        out.append((l1, l2, s, r2))
    return out


def _boundaries(own_even, own_odd, got_even, got_odd, bnd, count):
    odd = lax.axis_index("row") % 2 == 1

    def read(ref):
        return [ref[pl.ds(k * TILES, count), :] for k in range(6)]

    oe, oo, ge, go = read(own_even), read(own_odd), read(got_even), read(got_odd)

    def pick(yes, no):
        return [jnp.where(odd, y, n) for y, n in zip(yes, no)]

    top = _junction(pick(ge, go), pick(oe, oo))
    low = _junction(pick(oo, oe), pick(go, ge))
    for level in range(3):
        for j in range(4):
            bnd[pl.ds((level * 4 + j) * count, count), :] = (top if j < 2 else low)[level][j]


def _rows_transform(tile, edge):
    row = lax.axis_index("row")
    sub = _sub()
    is7, is0 = sub == 7, sub == 0
    mir7 = is7 & (row == lax.axis_size("row") - 1)
    mir0 = is0 & (row == 0)
    odd = (sub & 1) == 1
    zero = jnp.zeros((8, LANES), F32)

    def up(v, level, j, mirror):
        return jnp.where(mir7, mirror, jnp.where(is7, edge(level, j), pltpu.roll(v, 7, 0)))

    def dn(v, level, j, mirror):
        return jnp.where(mir0, mirror, jnp.where(is0, edge(level, j), pltpu.roll(v, 1, 0)))

    a, b, c, d = tile
    c1 = c + ALPHA * (a + b)
    d1 = d + ALPHA * (b + up(a, 0, 2, b))
    a1 = a + BETA * (dn(d1, 0, 0, c1) + c1)
    b1 = b + BETA * (c1 + d1)
    c2 = c1 + GAMMA * (a1 + b1)
    d2 = d1 + GAMMA * (b1 + up(a1, 0, 3, b1))
    a = (a1 + DELTA * (dn(d2, 0, 1, c2) + c2)) * SCALE_LOW
    b = (b1 + DELTA * (c2 + d2)) * SCALE_LOW
    v = [a, b, c2 * SCALE_HIGH, d2 * SCALE_HIGH]
    b1 = b + ALPHA * (a + up(a, 1, 2, a))
    a1 = a + BETA * (dn(b1, 1, 0, b1) + b1)
    b2 = b1 + GAMMA * (a1 + up(a1, 1, 3, a1))
    x = (a1 + DELTA * (dn(b2, 1, 1, b2) + b2)) * SCALE_LOW
    v += [x, b2 * SCALE_HIGH]
    for ka, kb, j in ((ALPHA, BETA, 0), (GAMMA, DELTA, 1)):
        back = pltpu.roll(x, 1, 0)
        x = x + jnp.where(odd, ka, zero) * (back + up(x, 2, 2 + j, back))
        ahead = pltpu.roll(x, 7, 0)
        x = x + jnp.where(odd, zero, kb) * (dn(x, 2, j, ahead) + ahead)
    v.append(x * jnp.where(odd, SCALE_HIGH, zero + SCALE_LOW))
    return v


def states_kernel(x_ref, even_ref, odd_ref, scr, sems):
    copies = [
        [
            _load(
                x_ref.at[img, rt],
                scr.at[pl.ds(img * CHUNKS, CHUNKS), pl.ds(rt * 8, 8), :],
                sems.at[img, rt],
            )
            for rt in range(4)
        ]
        for img in range(IMAGES)
    ]

    def run(to_end, to_start):
        for img in range(IMAGES):
            for copy in copies[img]:
                copy.wait()
            for c in range(CHUNKS):
                t = tile_row(img, c)
                end, start = _states_of(_rows_of(scr, img * CHUNKS + c))
                for k in range(6):
                    to_end[pl.ds(k * TILES + t, 1), :] = end[k]
                    to_start[pl.ds(k * TILES + t, 1), :] = start[k]

    is_odd = lax.axis_index("row") % 2 == 1
    pl.when(is_odd)(lambda: run(odd_ref, even_ref))
    pl.when(jnp.logical_not(is_odd))(lambda: run(even_ref, odd_ref))


def edges_kernel(x_ref, own_even, own_odd, got_even, got_odd, v_ref, even_ref, odd_ref, bnd):
    _boundaries(own_even, own_odd, got_even, got_odd, bnd, EDGES)
    lane = _lane()
    zero = jnp.zeros((8, LANES), F32)
    tiles = []
    for t in range(EDGES):

        def edge(level, j, t=t):
            return jnp.broadcast_to(bnd[pl.ds((level * 4 + j) * EDGES + t, 1), :], (8, LANES))

        column = (t % IMAGES) * CHUNKS + (t // IMAGES) * (CHUNKS - 1)
        v = _rows_transform(_rows_of(x_ref, column), edge)
        for k in range(7):
            v_ref[t, k] = v[k]
        tiles.append(v)
    is_odd = lax.axis_index("col") % 2 == 1
    for n, (base, count, width) in enumerate(KINDS):
        to_left, to_right = zero, zero
        for img in range(IMAGES):
            for q in range(count):
                slot = (img * count + q) * width
                here = (lane >= slot) & (lane < slot + width)
                start, end = tiles[img][base + q], tiles[IMAGES + img][base + q]
                if slot:
                    start = pltpu.roll(start, slot, 1)
                if (slot + width) % LANES:
                    end = pltpu.roll(end, slot + width, 1)
                to_left = jnp.where(here, start, to_left)
                to_right = jnp.where(here, end, to_right)
        even_ref[pl.ds(8 * n, 8), :] = jnp.where(is_odd, to_left, to_right)
        odd_ref[pl.ds(8 * n, 8), :] = jnp.where(is_odd, to_right, to_left)


def _split(x):
    high = x.astype(jnp.bfloat16)
    return high, (x - high.astype(F32)).astype(jnp.bfloat16)


def _dot(x, w):
    return jnp.dot(x, w, preferred_element_type=F32)


def main_kernel(later_ref, w_ref, x_ref, own_even, own_odd, got_even, got_odd, out_ref, edge_ref, scr, lh1, ll1, lh2, ll2, lh3, ll3, bnd, sems):
    del later_ref
    _boundaries(own_even, own_odd, got_even, got_odd, bnd, TILES)
    lane = _lane()
    low_half = lane < HALF
    lhs = ((lh1, ll1), (lh2, ll2), (lh3, ll3))

    def build(pair):
        before = None
        for c in range(CHUNKS + 1):
            now = before
            if c < CHUNKS:
                now = []
                for img in pair:

                    def edge(level, j, t=tile_row(img, c)):
                        return jnp.broadcast_to(bnd[pl.ds((level * 4 + j) * TILES + t, 1), :], (8, LANES))

                    v = _rows_transform(_rows_of(x_ref, img * CHUNKS + c), edge)
                    now.append([pltpu.roll(tile, HALF, 1) for tile in v])
            if before is None:
                before = now
            halves = [[jnp.where(low_half, p, q) for p, q in zip(ps, qs)] for ps, qs in zip(before, now)]
            rows1 = [tile for half in halves for tile in half[:4]]
            rows2 = [tile for half in halves for tile in half[4:6]]
            rows3 = [half[6] for half in halves]
            for (high_ref, low_ref), rows in zip(lhs, (rows1, rows2, rows3)):
                high, low = _split(jnp.concatenate(rows, axis=0))
                n = 8 * len(rows)
                for ref, part in ((high_ref, high), (low_ref, low)):
                    if c < CHUNKS:
                        ref[pl.ds(c * n, n), pl.ds(0, LANES)] = part
                    if c:
                        ref[pl.ds((c - 1) * n, n), pl.ds(LANES, LANES)] = part
            before = now

    def multiply(pair):
        outs = []
        for kind, (high_ref, low_ref) in enumerate(lhs):
            both = _dot(high_ref[...], w_ref[kind])
            outs.append(both[:, :LANES] + both[:, LANES:] + _dot(low_ref[...], w_ref[kind, :, :LANES]))
        for c in range(CHUNKS):
            for i, img in enumerate(pair):
                for q in range(4):
                    at = (c * 2 + i) * 32 + q * 8
                    val = outs[0][at : at + 8]
                    if q < 2:
                        at = (c * 2 + i) * 16 + q * 8
                        val = jnp.where((lane & 1) == 0, outs[1][at : at + 8], val)
                    if q < 1:
                        at = (c * 2 + i) * 8
                        val = jnp.where((lane & 3) == 0, outs[2][at : at + 8], val)
                    scr[img * CHUNKS + c, pl.ds(OFFSETS[q], 8, stride=4), :] = val

    stores = []
    for pair in ((0, 1), (2, 3)):
        build(pair)
        multiply(pair)
        for img in pair:
            for side, chunk in enumerate((0, CHUNKS - 1)):
                edge_ref[side * IMAGES + img] = scr[img * CHUNKS + chunk]
            for rt in range(4):
                stores.append(
                    _load(
                        scr.at[pl.ds(img * CHUNKS + 1, CHUNKS - 2), pl.ds(rt * 8, 8), :],
                        out_ref.at[img, rt, pl.ds(1, CHUNKS - 2)],
                        sems.at[img, rt],
                    )
                )
    for copy in stores:
        copy.wait()


def patch_kernel(w_ref, v_ref, edge_in, got_even, got_odd, dest_ref, out_ref, scr, sems):
    del dest_ref
    col = lax.axis_index("col")
    is_odd = col % 2 == 1
    which = (jnp.where(col == 0, 1, 0), jnp.where(col == lax.axis_size("col") - 1, 2, 0))
    lane = _lane()
    low_half = lane < HALF
    windows = [[[], [], []], [[], [], []]]
    for n, (base, count, width) in enumerate(KINDS):
        via_even, via_odd = got_even[pl.ds(8 * n, 8), :], got_odd[pl.ds(8 * n, 8), :]
        got = (jnp.where(is_odd, via_even, via_odd), jnp.where(is_odd, via_odd, via_even))
        for img in range(IMAGES):
            for q in range(count):
                slot = (img * count + q) * width
                for side, shift in ((0, HALF - slot - width), (1, HALF - slot)):
                    halo = pltpu.roll(got[side], shift % LANES, 1) if shift % LANES else got[side]
                    own = pltpu.roll(v_ref[side * IMAGES + img, base + q], HALF, 1)
                    first, second = (halo, own) if side == 0 else (own, halo)
                    windows[side][n].append(jnp.where(low_half, first, second))
    copies = []
    for side in range(2):
        outs = []
        for n in range(3):
            x = jnp.concatenate(windows[side][n], axis=0)
            y = _dot(jnp.concatenate(_split(x), axis=1), w_ref[which[side], n])
            outs.append(y[:, :LANES] + y[:, LANES:])
        inside = lane < PATCH if side == 0 else lane >= LANES - PATCH
        for img in range(IMAGES):
            t = side * IMAGES + img
            for q in range(4):
                at = (img * 4 + q) * 8
                new = outs[0][at : at + 8]
                if q < 2:
                    at = (img * 2 + q) * 8
                    new = jnp.where((lane & 1) == 0, outs[1][at : at + 8], new)
                if q < 1:
                    new = jnp.where((lane & 3) == 0, outs[2][img * 8 : img * 8 + 8], new)
                where = (t, pl.ds(OFFSETS[q], 8, stride=4), slice(None))
                scr[where] = jnp.where(inside, pltpu.roll(new, HALF, 1), edge_in[where])
            column = scr.reshape(EDGES, 4, 8, LANES).at[t]
            copies.append(_load(column, out_ref.at[img, :, (CHUNKS - 1) * side], sems.at[t]))
    for copy in copies:
        copy.wait()


def swap(axis, even, odd):
    n = lax.axis_size(axis)
    even_pairs = [(i, i ^ 1) for i in range(n)]
    odd_pairs = [(i, i + 1 if i % 2 else i - 1) for i in range(1, n - 1)] + [(0, 0), (n - 1, n - 1)]
    via_odd = lax.ppermute(odd, axis, odd_pairs)
    via_even = lax.ppermute(even, axis, even_pairs)
    return near(via_even), near(via_odd)


def near(value):
    return pltpu.with_memory_space_constraint(value, pltpu.VMEM)


def held(*dims):
    return pltpu.VMEM(dims, F32)


VMEM = pl.BlockSpec(memory_space=pltpu.VMEM)
ANY = pl.BlockSpec(memory_space=pl.ANY)


def shape(*dims):
    return jax.ShapeDtypeStruct(dims, F32)


def transform(images):
    x = images.reshape(IMAGES, 4, 8, CHUNKS, LANES).transpose(0, 1, 3, 2, 4)
    dma = pltpu.SemaphoreType.DMA
    row_even, row_odd, block = pl.pallas_call(
        states_kernel,
        out_shape=(held(6 * TILES, LANES), held(6 * TILES, LANES), held(TILES, ROWS, LANES)),
        in_specs=[ANY],
        out_specs=(VMEM,) * 3,
        scratch_shapes=[dma((IMAGES, 4))],
        compiler_params=pltpu.CompilerParams(vmem_limit_bytes=8 << 20),
        name="row_states",
    )(pltpu.with_memory_space_constraint(x, pltpu.HBM))
    got_even, got_odd = swap("row", row_even, row_odd)
    rows = (near(block), near(row_even), near(row_odd), got_even, got_odd)
    v_edge, col_even, col_odd = pl.pallas_call(
        edges_kernel,
        out_shape=(held(EDGES, 7, 8, LANES), held(24, LANES), held(24, LANES)),
        in_specs=[VMEM] * 5,
        out_specs=(VMEM,) * 3,
        scratch_shapes=[pltpu.VMEM((12 * EDGES, LANES), F32)],
        compiler_params=pltpu.CompilerParams(vmem_limit_bytes=8 << 20),
        name="edge_rows",
    )(*rows)
    edge_matrices = near(jnp.asarray(EDGE))
    halo_even, halo_odd = swap("col", col_even, col_odd)
    out, out_edge = pl.pallas_call(
        main_kernel,
        out_shape=(shape(IMAGES, 4, CHUNKS, 8, LANES), held(EDGES, ROWS, LANES)),
        in_specs=[VMEM] * 7,
        out_specs=(ANY, VMEM),
        scratch_shapes=[
            pltpu.VMEM((TILES, ROWS, LANES), F32),
            *(pltpu.VMEM((CHUNKS * n, 2 * LANES), jnp.bfloat16) for n in (64, 64, 32, 32, 16, 16)),
            pltpu.VMEM((12 * TILES, LANES), F32),
            dma((IMAGES, 4)),
        ],
        cost_estimate=pl.CostEstimate(flops=40_000_000, transcendentals=0, bytes_accessed=2_000_000),
        compiler_params=pltpu.CompilerParams(vmem_limit_bytes=24 << 20),
        name="interior",
    )(edge_matrices, near(jnp.asarray(LINE)), *rows)
    out = pl.pallas_call(
        patch_kernel,
        out_shape=shape(IMAGES, 4, CHUNKS, 8, LANES),
        in_specs=[VMEM] * 5 + [ANY],
        out_specs=ANY,
        input_output_aliases={5: 0},
        scratch_shapes=[pltpu.VMEM((EDGES, ROWS, LANES), F32), dma((EDGES,))],
        compiler_params=pltpu.CompilerParams(vmem_limit_bytes=8 << 20),
        name="edge_columns",
    )(edge_matrices, near(v_edge), near(out_edge), halo_even, halo_odd, out)
    return out.transpose(0, 1, 3, 2, 4).reshape(IMAGES, ROWS, CHUNKS * LANES)


def solution(mesh):
    return jax.shard_map(
        transform,
        mesh=mesh,
        in_specs=(P(None, "row", "col"),),
        out_specs=P(None, "row", "col"),
        check_vma=False,
    )
```

```python
import jax
import jax.numpy as jnp
import numpy as np
from jax import lax
from jax.experimental import pallas as pl
from jax.experimental.pallas import tpu as pltpu
from jax.sharding import PartitionSpec as P


ALPHA = -1.586134342
BETA = -0.05298011854
GAMMA = 0.8829110762
DELTA = 0.4435068522
SCALE_HIGH = 1.230174105
SCALE_LOW = 1.0 / 1.230174105

IMAGES = 4
ROWS = 32
CHUNKS = 16
TILES = IMAGES * CHUNKS
LANES = 128
EDGES = 2 * IMAGES
HALF = LANES // 2
PATCH = 32
F32 = jnp.float32
OFFSETS = (0, 2, 1, 3)
KINDS = ((0, 4, 8), (4, 2, 16), (6, 1, 32))


def tile_row(img, chunk):
    place = 0 if chunk == 0 else 1 if chunk == CHUNKS - 1 else chunk + 1
    return place * IMAGES + img


def _lift(x, left, right):
    s, d = x[0::2], x[1::2]
    m = len(s)
    d = [d[i] + ALPHA * (s[i] + (s[i + 1] if i + 1 < m else right[0])) for i in range(m)]
    s = [s[i] + BETA * ((d[i - 1] if i else left[0]) + d[i]) for i in range(m)]
    d = [d[i] + GAMMA * (s[i] + (s[i + 1] if i + 1 < m else right[1])) for i in range(m)]
    s = [s[i] + DELTA * ((d[i - 1] if i else left[1]) + d[i]) for i in range(m)]
    return [v * SCALE_LOW for v in s], [v * SCALE_HIGH for v in d]


def _states(x):
    p = x[-1] + ALPHA * x[-2]
    t = x[-2] + BETA * (x[-3] + ALPHA * (x[-4] + x[-2]))
    s = x[0]
    u = x[0] + BETA * (x[1] + ALPHA * (x[0] + x[2]))
    return p, t, s, u


def _responses():
    zero = (0.0, 0.0)
    end, start = {}, {}
    for level in (1, 2):
        for j in range(2):
            unit = (1.0, 0.0) if j == 0 else (0.0, 1.0)
            for table, left, right, pick in ((end, zero, unit, 0), (start, unit, zero, 2)):
                band = [0.0] * (ROWS >> (level - 1))
                low, _ = _lift(band, left, right)
                for into in range(level + 1, 4):
                    table[level, into, j] = _states(low)[pick : pick + 2]
                    low, _ = _lift(low, zero, zero)
    return end, start


END, START = _responses()


def _levels(x, mirror):
    out, st = [], 1
    for _ in range(3):
        s, d = list(x[0::2]), list(x[1::2])
        m = len(s)
        for odd, even in ((ALPHA, BETA), (GAMMA, DELTA)):
            for i in range(m):
                after = s[i + 1] if i + 1 < m else 0.0
                if mirror and mirror[0] == 1 and (2 * i + 2) * st > mirror[1]:
                    after = s[i]
                d[i] = d[i] + odd * (s[i] + after)
            for i in range(m):
                before = d[i - 1] if i else 0.0
                if mirror and mirror[0] == 0 and 2 * i * st == mirror[1]:
                    before = d[i]
                s[i] = s[i] + even * (before + d[i])
        s, d = [v * SCALE_LOW for v in s], [v * SCALE_HIGH for v in d]
        now = {2 * i * st: v for i, v in enumerate(s)}
        now.update({(2 * i + 1) * st: v for i, v in enumerate(d)})
        out.append(now)
        x, st = s, 2 * st
    return out


def _matrices(span, taken, given, mirror=None):
    table = np.zeros((3, taken[1], given[1]))
    for k in range(taken[1]):
        at = taken[0] + k
        if mirror and (at < mirror[1] if mirror[0] == 0 else at > mirror[1]):
            continue
        x = [0.0] * span
        x[at] = 1.0
        for level, values in enumerate(_levels(x, mirror)):
            for n in range(given[1]):
                table[level, k, n] = values.get(given[0] + n, 0.0)
    return table.astype(np.float32)


def _parts(table):
    high = table.astype(jnp.bfloat16)
    return high, (table - high.astype(np.float32)).astype(jnp.bfloat16)


def _line_matrices():
    high, low = _parts(_matrices(4 * LANES, (LANES, 2 * LANES), (LANES + HALF, LANES)))
    return np.concatenate([high, low], axis=2)


def _edge_matrices():
    out = []
    for mirror in (None, (0, 2 * LANES), (1, 2 * LANES - 1)):
        high, low = _parts(_matrices(4 * LANES, (2 * LANES - HALF, LANES), (2 * LANES - HALF, LANES), mirror))
        top = np.concatenate([high, low], axis=2)
        bottom = np.concatenate([high, np.zeros_like(high)], axis=2)
        out.append(np.concatenate([top, bottom], axis=1))
    return np.stack(out)


LINE = _line_matrices()
EDGE = _edge_matrices()


def _sub():
    return lax.broadcasted_iota(jnp.int32, (8, LANES), 0)


def _lane():
    return lax.broadcasted_iota(jnp.int32, (8, LANES), 1)


def _load(src, dst, sem):
    copy = pltpu.make_async_copy(src, dst, sem)
    copy.start()
    return copy


def _rows_of(ref, t):
    return [ref[t, pl.ds(q, 8, stride=4), :] for q in OFFSETS]


def _states_of(tile):
    sub = _sub()
    is7, is0 = sub == 7, sub == 0
    zero = jnp.zeros((8, LANES), F32)

    def up(v):
        return jnp.where(is7, zero, pltpu.roll(v, 7, 0))

    def dn(v):
        return jnp.where(is0, zero, pltpu.roll(v, 1, 0))

    a, b, c, d = tile
    c1 = c + ALPHA * (a + b)
    end = [(d + ALPHA * b)[7:8], (b + BETA * c1)[7:8]]
    start = [a[0:1], (a + BETA * c1)[0:1]]
    d1 = d + ALPHA * (b + up(a))
    a1 = a + BETA * (dn(d1) + c1)
    b1 = b + BETA * (c1 + d1)
    c2 = c1 + GAMMA * (a1 + b1)
    d2 = d1 + GAMMA * (b1 + up(a1))
    a = (a1 + DELTA * (dn(d2) + c2)) * SCALE_LOW
    b = (b1 + DELTA * (c2 + d2)) * SCALE_LOW
    b1 = b + ALPHA * (a + up(a))
    rb = dn(b1)
    end += [(b + ALPHA * a)[7:8], (a + BETA * rb)[7:8]]
    start += [a[0:1], (a + BETA * b1)[0:1]]
    a1 = a + BETA * (rb + b1)
    b2 = b1 + GAMMA * (a1 + up(a1))
    x = (a1 + DELTA * (dn(b2) + b2)) * SCALE_LOW
    back = pltpu.roll(x, 1, 0)
    x1 = x + ALPHA * (back + pltpu.roll(x, 7, 0))
    end += [(x + ALPHA * back)[7:8], (x + BETA * pltpu.roll(x1, 1, 0))[6:7]]
    start += [x[0:1], (x + BETA * pltpu.roll(x1, 7, 0))[0:1]]
    return end, start


def _junction(ends, starts):
    out = []
    for level in (1, 2, 3):
        p, t = ends[2 * level - 2], ends[2 * level - 1]
        s, u = starts[2 * level - 2], starts[2 * level - 1]
        for prior in range(1, level):
            l1, l2, r1, r2 = out[prior - 1]
            e0, e1 = END[prior, level, 0], END[prior, level, 1]
            s0, s1 = START[prior, level, 0], START[prior, level, 1]
            p = p + e0[0] * r1 + e1[0] * r2
            t = t + e0[1] * r1 + e1[1] * r2
            s = s + s0[0] * l1 + s1[0] * l2
            u = u + s0[1] * l1 + s1[1] * l2
        l1 = p + ALPHA * s
        r2 = u + BETA * l1
        l2 = l1 + GAMMA * (t + BETA * l1 + r2)
        out.append((l1, l2, s, r2))
    return out


def _boundaries(own_even, own_odd, got_even, got_odd, bnd, count):
    odd = lax.axis_index("row") % 2 == 1

    def read(ref):
        return [ref[pl.ds(k * TILES, count), :] for k in range(6)]

    oe, oo, ge, go = read(own_even), read(own_odd), read(got_even), read(got_odd)

    def pick(yes, no):
        return [jnp.where(odd, y, n) for y, n in zip(yes, no)]

    top = _junction(pick(ge, go), pick(oe, oo))
    low = _junction(pick(oo, oe), pick(go, ge))
    for level in range(3):
        for j in range(4):
            bnd[pl.ds((level * 4 + j) * count, count), :] = (top if j < 2 else low)[level][j]


def _rows_transform(tile, edge):
    row = lax.axis_index("row")
    sub = _sub()
    is7, is0 = sub == 7, sub == 0
    mir7 = is7 & (row == lax.axis_size("row") - 1)
    mir0 = is0 & (row == 0)
    odd = (sub & 1) == 1
    zero = jnp.zeros((8, LANES), F32)

    def up(v, level, j, mirror):
        return jnp.where(mir7, mirror, jnp.where(is7, edge(level, j), pltpu.roll(v, 7, 0)))

    def dn(v, level, j, mirror):
        return jnp.where(mir0, mirror, jnp.where(is0, edge(level, j), pltpu.roll(v, 1, 0)))

    a, b, c, d = tile
    c1 = c + ALPHA * (a + b)
    d1 = d + ALPHA * (b + up(a, 0, 2, b))
    a1 = a + BETA * (dn(d1, 0, 0, c1) + c1)
    b1 = b + BETA * (c1 + d1)
    c2 = c1 + GAMMA * (a1 + b1)
    d2 = d1 + GAMMA * (b1 + up(a1, 0, 3, b1))
    a = (a1 + DELTA * (dn(d2, 0, 1, c2) + c2)) * SCALE_LOW
    b = (b1 + DELTA * (c2 + d2)) * SCALE_LOW
    v = [a, b, c2 * SCALE_HIGH, d2 * SCALE_HIGH]
    b1 = b + ALPHA * (a + up(a, 1, 2, a))
    a1 = a + BETA * (dn(b1, 1, 0, b1) + b1)
    b2 = b1 + GAMMA * (a1 + up(a1, 1, 3, a1))
    x = (a1 + DELTA * (dn(b2, 1, 1, b2) + b2)) * SCALE_LOW
    v += [x, b2 * SCALE_HIGH]
    for ka, kb, j in ((ALPHA, BETA, 0), (GAMMA, DELTA, 1)):
        back = pltpu.roll(x, 1, 0)
        x = x + jnp.where(odd, ka, zero) * (back + up(x, 2, 2 + j, back))
        ahead = pltpu.roll(x, 7, 0)
        x = x + jnp.where(odd, zero, kb) * (dn(x, 2, j, ahead) + ahead)
    v.append(x * jnp.where(odd, SCALE_HIGH, zero + SCALE_LOW))
    return v


def states_kernel(x_ref, even_ref, odd_ref, scr, sems):
    copies = [
        [
            _load(
                x_ref.at[img, rt],
                scr.at[pl.ds(img * CHUNKS, CHUNKS), pl.ds(rt * 8, 8), :],
                sems.at[img, rt],
            )
            for rt in range(4)
        ]
        for img in range(IMAGES)
    ]

    def run(to_end, to_start):
        for img in range(IMAGES):
            for copy in copies[img]:
                copy.wait()
            for c in range(CHUNKS):
                t = tile_row(img, c)
                end, start = _states_of(_rows_of(scr, img * CHUNKS + c))
                for k in range(6):
                    to_end[pl.ds(k * TILES + t, 1), :] = end[k]
                    to_start[pl.ds(k * TILES + t, 1), :] = start[k]

    is_odd = lax.axis_index("row") % 2 == 1
    pl.when(is_odd)(lambda: run(odd_ref, even_ref))
    pl.when(jnp.logical_not(is_odd))(lambda: run(even_ref, odd_ref))


def edges_kernel(x_ref, own_even, own_odd, got_even, got_odd, v_ref, even_ref, odd_ref, bnd):
    _boundaries(own_even, own_odd, got_even, got_odd, bnd, EDGES)
    lane = _lane()
    zero = jnp.zeros((8, LANES), F32)
    tiles = []
    for t in range(EDGES):

        def edge(level, j, t=t):
            return jnp.broadcast_to(bnd[pl.ds((level * 4 + j) * EDGES + t, 1), :], (8, LANES))

        column = (t % IMAGES) * CHUNKS + (t // IMAGES) * (CHUNKS - 1)
        v = _rows_transform(_rows_of(x_ref, column), edge)
        for k in range(7):
            v_ref[t, k] = v[k]
        tiles.append(v)
    is_odd = lax.axis_index("col") % 2 == 1
    for n, (base, count, width) in enumerate(KINDS):
        to_left, to_right = zero, zero
        for img in range(IMAGES):
            for q in range(count):
                slot = (img * count + q) * width
                here = (lane >= slot) & (lane < slot + width)
                start, end = tiles[img][base + q], tiles[IMAGES + img][base + q]
                if slot:
                    start = pltpu.roll(start, slot, 1)
                if (slot + width) % LANES:
                    end = pltpu.roll(end, slot + width, 1)
                to_left = jnp.where(here, start, to_left)
                to_right = jnp.where(here, end, to_right)
        even_ref[pl.ds(8 * n, 8), :] = jnp.where(is_odd, to_left, to_right)
        odd_ref[pl.ds(8 * n, 8), :] = jnp.where(is_odd, to_right, to_left)


def _split(x):
    high = x.astype(jnp.bfloat16)
    return high, (x - high.astype(F32)).astype(jnp.bfloat16)


def _dot(x, w):
    return jnp.dot(x, w, preferred_element_type=F32)


def interior(pairs, later_ref, w_ref, x_ref, own_even, own_odd, got_even, got_odd, edge_ref, scr, lh1, ll1, lh2, ll2, lh3, ll3, bnd, done):
    del later_ref
    _boundaries(own_even, own_odd, got_even, got_odd, bnd, TILES)
    lane = _lane()
    low_half = lane < HALF
    lhs = ((lh1, ll1), (lh2, ll2), (lh3, ll3))

    def build(pair):
        before = None
        for c in range(CHUNKS + 1):
            now = before
            if c < CHUNKS:
                now = []
                for img in pair:

                    def edge(level, j, t=tile_row(img, c)):
                        return jnp.broadcast_to(bnd[pl.ds((level * 4 + j) * TILES + t, 1), :], (8, LANES))

                    v = _rows_transform(_rows_of(x_ref, img * CHUNKS + c), edge)
                    now.append([pltpu.roll(tile, HALF, 1) for tile in v])
            if before is None:
                before = now
            halves = [[jnp.where(low_half, p, q) for p, q in zip(ps, qs)] for ps, qs in zip(before, now)]
            rows1 = [tile for half in halves for tile in half[:4]]
            rows2 = [tile for half in halves for tile in half[4:6]]
            rows3 = [half[6] for half in halves]
            for (high_ref, low_ref), rows in zip(lhs, (rows1, rows2, rows3)):
                high, low = _split(jnp.concatenate(rows, axis=0))
                n = 8 * len(rows)
                for ref, part in ((high_ref, high), (low_ref, low)):
                    if c < CHUNKS:
                        ref[pl.ds(c * n, n), pl.ds(0, LANES)] = part
                    if c:
                        ref[pl.ds((c - 1) * n, n), pl.ds(LANES, LANES)] = part
            before = now

    def multiply(pair):
        outs = []
        for kind, (high_ref, low_ref) in enumerate(lhs):
            both = _dot(high_ref[...], w_ref[kind])
            outs.append(both[:, :LANES] + both[:, LANES:] + _dot(low_ref[...], w_ref[kind, :, :LANES]))
        for c in range(CHUNKS):
            for i, img in enumerate(pair):
                for q in range(4):
                    at = (c * 2 + i) * 32 + q * 8
                    val = outs[0][at : at + 8]
                    if q < 2:
                        at = (c * 2 + i) * 16 + q * 8
                        val = jnp.where((lane & 1) == 0, outs[1][at : at + 8], val)
                    if q < 1:
                        at = (c * 2 + i) * 8
                        val = jnp.where((lane & 3) == 0, outs[2][at : at + 8], val)
                    scr[img * CHUNKS + c, pl.ds(OFFSETS[q], 8, stride=4), :] = val

    for pair in pairs:
        build(pair)
        multiply(pair)
        for img in pair:
            for side, chunk in enumerate((0, CHUNKS - 1)):
                edge_ref[side * IMAGES + img] = scr[img * CHUNKS + chunk]
        done(pair)


def is_early():
    return lax.axis_index("col") % 8 == 0


FIRST, SECOND = (0, 1), (2, 3)


def early_kernel(*refs):
    pl.when(is_early())(lambda: interior((FIRST,), *refs, lambda pair: None))


def late_kernel(*refs):
    ins, (_, kept, out_ref, edge_ref, scr, *rest, sems) = refs[:7], refs[7:]

    def store(pair, source):
        return [
            _load(
                source.at[pl.ds(img * CHUNKS + 1, CHUNKS - 2), pl.ds(rt * 8, 8), :],
                out_ref.at[img, rt, pl.ds(1, CHUNKS - 2)],
                sems.at[img, rt],
            )
            for img in pair
            for rt in range(4)
        ]

    def run(pairs, stores):
        interior(pairs, *ins, edge_ref, scr, *rest, lambda pair: stores.extend(store(pair, scr)))
        for copy in stores:
            copy.wait()

    pl.when(is_early())(lambda: run((SECOND,), store(FIRST, kept)))
    pl.when(jnp.logical_not(is_early()))(lambda: run((FIRST, SECOND), []))


def patch_kernel(w_ref, v_ref, edge_in, got_even, got_odd, dest_ref, out_ref, scr, sems):
    del dest_ref
    col = lax.axis_index("col")
    is_odd = col % 2 == 1
    which = (jnp.where(col == 0, 1, 0), jnp.where(col == lax.axis_size("col") - 1, 2, 0))
    lane = _lane()
    low_half = lane < HALF
    windows = [[[], [], []], [[], [], []]]
    for n, (base, count, width) in enumerate(KINDS):
        via_even, via_odd = got_even[pl.ds(8 * n, 8), :], got_odd[pl.ds(8 * n, 8), :]
        got = (jnp.where(is_odd, via_even, via_odd), jnp.where(is_odd, via_odd, via_even))
        for img in range(IMAGES):
            for q in range(count):
                slot = (img * count + q) * width
                for side, shift in ((0, HALF - slot - width), (1, HALF - slot)):
                    halo = pltpu.roll(got[side], shift % LANES, 1) if shift % LANES else got[side]
                    own = pltpu.roll(v_ref[side * IMAGES + img, base + q], HALF, 1)
                    first, second = (halo, own) if side == 0 else (own, halo)
                    windows[side][n].append(jnp.where(low_half, first, second))
    copies = []
    for side in range(2):
        outs = []
        for n in range(3):
            x = jnp.concatenate(windows[side][n], axis=0)
            y = _dot(jnp.concatenate(_split(x), axis=1), w_ref[which[side], n])
            outs.append(y[:, :LANES] + y[:, LANES:])
        inside = lane < PATCH if side == 0 else lane >= LANES - PATCH
        for img in range(IMAGES):
            t = side * IMAGES + img
            for q in range(4):
                at = (img * 4 + q) * 8
                new = outs[0][at : at + 8]
                if q < 2:
                    at = (img * 2 + q) * 8
                    new = jnp.where((lane & 1) == 0, outs[1][at : at + 8], new)
                if q < 1:
                    new = jnp.where((lane & 3) == 0, outs[2][img * 8 : img * 8 + 8], new)
                where = (t, pl.ds(OFFSETS[q], 8, stride=4), slice(None))
                scr[where] = jnp.where(inside, pltpu.roll(new, HALF, 1), edge_in[where])
            column = scr.reshape(EDGES, 4, 8, LANES).at[t]
            copies.append(_load(column, out_ref.at[img, :, (CHUNKS - 1) * side], sems.at[t]))
    for copy in copies:
        copy.wait()


def pairs(axis):
    n = lax.axis_size(axis)
    even_pairs = [(i, i ^ 1) for i in range(n)]
    odd_pairs = [(i, i + 1 if i % 2 else i - 1) for i in range(1, n - 1)] + [(0, 0), (n - 1, n - 1)]
    return even_pairs, odd_pairs


def swap(axis, even, odd):
    even_pairs, odd_pairs = pairs(axis)
    via_odd = lax.ppermute(odd, axis, odd_pairs)
    via_even = lax.ppermute(even, axis, even_pairs)
    return near(via_even), near(via_odd)


def near(value):
    return pltpu.with_memory_space_constraint(value, pltpu.VMEM)


def held(*dims):
    return pltpu.VMEM(dims, F32)


VMEM = pl.BlockSpec(memory_space=pltpu.VMEM)
ANY = pl.BlockSpec(memory_space=pl.ANY)


def shape(*dims):
    return jax.ShapeDtypeStruct(dims, F32)


def transform(images):
    x = images.reshape(IMAGES, 4, 8, CHUNKS, LANES).transpose(0, 1, 3, 2, 4)
    dma = pltpu.SemaphoreType.DMA
    row_even, row_odd, block = pl.pallas_call(
        states_kernel,
        out_shape=(held(6 * TILES, LANES), held(6 * TILES, LANES), held(TILES, ROWS, LANES)),
        in_specs=[ANY],
        out_specs=(VMEM,) * 3,
        scratch_shapes=[dma((IMAGES, 4))],
        compiler_params=pltpu.CompilerParams(vmem_limit_bytes=8 << 20),
        name="row_states",
    )(pltpu.with_memory_space_constraint(x, pltpu.HBM))
    got_even, got_odd = swap("row", row_even, row_odd)
    rows = (near(block), near(row_even), near(row_odd), got_even, got_odd)
    v_edge, col_even, col_odd = pl.pallas_call(
        edges_kernel,
        out_shape=(held(EDGES, 7, 8, LANES), held(24, LANES), held(24, LANES)),
        in_specs=[VMEM] * 5,
        out_specs=(VMEM,) * 3,
        scratch_shapes=[pltpu.VMEM((12 * EDGES, LANES), F32)],
        compiler_params=pltpu.CompilerParams(vmem_limit_bytes=8 << 20),
        name="edge_rows",
    )(*rows)
    edge_matrices = near(jnp.asarray(EDGE))
    operands = (edge_matrices, near(jnp.asarray(LINE)), *rows)
    work = [
        *(pltpu.VMEM((CHUNKS * n, 2 * LANES), jnp.bfloat16) for n in (64, 64, 32, 32, 16, 16)),
        pltpu.VMEM((12 * TILES, LANES), F32),
    ]
    settings = dict(
        cost_estimate=pl.CostEstimate(flops=40_000_000, transcendentals=0, bytes_accessed=2_000_000),
        compiler_params=pltpu.CompilerParams(vmem_limit_bytes=24 << 20),
    )
    even_pairs, odd_pairs = pairs("col")
    halo_even = lax.ppermute(col_even, "col", even_pairs)
    out_edge, kept = pl.pallas_call(
        early_kernel,
        out_shape=(held(EDGES, ROWS, LANES), held(TILES, ROWS, LANES)),
        in_specs=[VMEM] * 7,
        out_specs=(VMEM, VMEM),
        scratch_shapes=work,
        name="interior_early",
        **settings,
    )(*operands)
    col_odd, out_edge = lax.optimization_barrier((col_odd, out_edge))
    halo_odd = lax.ppermute(near(col_odd), "col", odd_pairs)
    out, out_edge = pl.pallas_call(
        late_kernel,
        out_shape=(shape(IMAGES, 4, CHUNKS, 8, LANES), held(EDGES, ROWS, LANES)),
        in_specs=[VMEM] * 9,
        out_specs=(ANY, VMEM),
        input_output_aliases={7: 1},
        scratch_shapes=[pltpu.VMEM((TILES, ROWS, LANES), F32), *work, dma((IMAGES, 4))],
        name="interior_late",
        **settings,
    )(*operands, near(out_edge), near(kept))
    halo_even, halo_odd = near(halo_even), near(halo_odd)
    out = pl.pallas_call(
        patch_kernel,
        out_shape=shape(IMAGES, 4, CHUNKS, 8, LANES),
        in_specs=[VMEM] * 5 + [ANY],
        out_specs=ANY,
        input_output_aliases={5: 0},
        scratch_shapes=[pltpu.VMEM((EDGES, ROWS, LANES), F32), dma((EDGES,))],
        compiler_params=pltpu.CompilerParams(vmem_limit_bytes=8 << 20),
        name="edge_columns",
    )(edge_matrices, near(v_edge), near(out_edge), halo_even, halo_odd, out)
    return out.transpose(0, 1, 3, 2, 4).reshape(IMAGES, ROWS, CHUNKS * LANES)


def solution(mesh):
    return jax.shard_map(
        transform,
        mesh=mesh,
        in_specs=(P(None, "row", "col"),),
        out_specs=P(None, "row", "col"),
        check_vma=False,
    )
```

```python
import jax
import jax.numpy as jnp
import numpy as np
from jax import lax
from jax.experimental import pallas as pl
from jax.experimental.pallas import tpu as pltpu
from jax.sharding import PartitionSpec as P


ALPHA = -1.586134342
BETA = -0.05298011854
GAMMA = 0.8829110762
DELTA = 0.4435068522
SCALE_HIGH = 1.230174105
SCALE_LOW = 1.0 / 1.230174105

IMAGES = 4
ROWS = 32
CHUNKS = 16
TILES = IMAGES * CHUNKS
LANES = 128
EDGES = 2 * IMAGES
HALF = LANES // 2
PATCH = 32
F32 = jnp.float32
OFFSETS = (0, 2, 1, 3)
KINDS = ((0, 4, 8), (4, 2, 16), (6, 1, 32))


def tile_row(img, chunk):
    place = 0 if chunk == 0 else 1 if chunk == CHUNKS - 1 else chunk + 1
    return place * IMAGES + img


def _lift(x, left, right):
    s, d = x[0::2], x[1::2]
    m = len(s)
    d = [d[i] + ALPHA * (s[i] + (s[i + 1] if i + 1 < m else right[0])) for i in range(m)]
    s = [s[i] + BETA * ((d[i - 1] if i else left[0]) + d[i]) for i in range(m)]
    d = [d[i] + GAMMA * (s[i] + (s[i + 1] if i + 1 < m else right[1])) for i in range(m)]
    s = [s[i] + DELTA * ((d[i - 1] if i else left[1]) + d[i]) for i in range(m)]
    return [v * SCALE_LOW for v in s], [v * SCALE_HIGH for v in d]


def _states(x):
    p = x[-1] + ALPHA * x[-2]
    t = x[-2] + BETA * (x[-3] + ALPHA * (x[-4] + x[-2]))
    s = x[0]
    u = x[0] + BETA * (x[1] + ALPHA * (x[0] + x[2]))
    return p, t, s, u


def _responses():
    zero = (0.0, 0.0)
    end, start = {}, {}
    for level in (1, 2):
        for j in range(2):
            unit = (1.0, 0.0) if j == 0 else (0.0, 1.0)
            for table, left, right, pick in ((end, zero, unit, 0), (start, unit, zero, 2)):
                band = [0.0] * (ROWS >> (level - 1))
                low, _ = _lift(band, left, right)
                for into in range(level + 1, 4):
                    table[level, into, j] = _states(low)[pick : pick + 2]
                    low, _ = _lift(low, zero, zero)
    return end, start


END, START = _responses()


def _levels(x, mirror):
    out, st = [], 1
    for _ in range(3):
        s, d = list(x[0::2]), list(x[1::2])
        m = len(s)
        for odd, even in ((ALPHA, BETA), (GAMMA, DELTA)):
            for i in range(m):
                after = s[i + 1] if i + 1 < m else 0.0
                if mirror and mirror[0] == 1 and (2 * i + 2) * st > mirror[1]:
                    after = s[i]
                d[i] = d[i] + odd * (s[i] + after)
            for i in range(m):
                before = d[i - 1] if i else 0.0
                if mirror and mirror[0] == 0 and 2 * i * st == mirror[1]:
                    before = d[i]
                s[i] = s[i] + even * (before + d[i])
        s, d = [v * SCALE_LOW for v in s], [v * SCALE_HIGH for v in d]
        now = {2 * i * st: v for i, v in enumerate(s)}
        now.update({(2 * i + 1) * st: v for i, v in enumerate(d)})
        out.append(now)
        x, st = s, 2 * st
    return out


def _matrices(span, taken, given, mirror=None):
    table = np.zeros((3, taken[1], given[1]))
    for k in range(taken[1]):
        at = taken[0] + k
        if mirror and (at < mirror[1] if mirror[0] == 0 else at > mirror[1]):
            continue
        x = [0.0] * span
        x[at] = 1.0
        for level, values in enumerate(_levels(x, mirror)):
            for n in range(given[1]):
                table[level, k, n] = values.get(given[0] + n, 0.0)
    return table.astype(np.float32)


def _parts(table):
    high = table.astype(jnp.bfloat16)
    return high, (table - high.astype(np.float32)).astype(jnp.bfloat16)


def _line_matrices():
    high, low = _parts(_matrices(4 * LANES, (LANES, 2 * LANES), (LANES + HALF, LANES)))
    return np.concatenate([high, low], axis=2)


def _edge_matrices():
    out = []
    for mirror in (None, (0, 2 * LANES), (1, 2 * LANES - 1)):
        table = _matrices(4 * LANES, (2 * LANES - HALF, LANES), (2 * LANES - HALF, LANES), mirror)
        high, low = _parts(np.roll(table, (HALF, HALF), axis=(1, 2)))
        top = np.concatenate([high, low], axis=2)
        bottom = np.concatenate([high, np.zeros_like(high)], axis=2)
        out.append(np.concatenate([top, bottom], axis=1))
    return np.stack(out)


LINE = _line_matrices()
EDGE = _edge_matrices()


def _sub():
    return lax.broadcasted_iota(jnp.int32, (8, LANES), 0)


def _lane():
    return lax.broadcasted_iota(jnp.int32, (8, LANES), 1)


def _load(src, dst, sem):
    copy = pltpu.make_async_copy(src, dst, sem)
    copy.start()
    return copy


def _rows_of(ref, t):
    return [ref[t, pl.ds(q, 8, stride=4), :] for q in OFFSETS]


def _states_of(tile):
    sub = _sub()
    is7, is0 = sub == 7, sub == 0
    zero = jnp.zeros((8, LANES), F32)

    def up(v):
        return jnp.where(is7, zero, pltpu.roll(v, 7, 0))

    def dn(v):
        return jnp.where(is0, zero, pltpu.roll(v, 1, 0))

    a, b, c, d = tile
    c1 = c + ALPHA * (a + b)
    end = [(d + ALPHA * b)[7:8], (b + BETA * c1)[7:8]]
    start = [a[0:1], (a + BETA * c1)[0:1]]
    d1 = d + ALPHA * (b + up(a))
    a1 = a + BETA * (dn(d1) + c1)
    b1 = b + BETA * (c1 + d1)
    c2 = c1 + GAMMA * (a1 + b1)
    d2 = d1 + GAMMA * (b1 + up(a1))
    a = (a1 + DELTA * (dn(d2) + c2)) * SCALE_LOW
    b = (b1 + DELTA * (c2 + d2)) * SCALE_LOW
    b1 = b + ALPHA * (a + up(a))
    rb = dn(b1)
    end += [(b + ALPHA * a)[7:8], (a + BETA * rb)[7:8]]
    start += [a[0:1], (a + BETA * b1)[0:1]]
    a1 = a + BETA * (rb + b1)
    b2 = b1 + GAMMA * (a1 + up(a1))
    x = (a1 + DELTA * (dn(b2) + b2)) * SCALE_LOW
    back = pltpu.roll(x, 1, 0)
    x1 = x + ALPHA * (back + pltpu.roll(x, 7, 0))
    end += [(x + ALPHA * back)[7:8], (x + BETA * pltpu.roll(x1, 1, 0))[6:7]]
    start += [x[0:1], (x + BETA * pltpu.roll(x1, 7, 0))[0:1]]
    return end, start


def _junction(ends, starts):
    out = []
    for level in (1, 2, 3):
        p, t = ends[2 * level - 2], ends[2 * level - 1]
        s, u = starts[2 * level - 2], starts[2 * level - 1]
        for prior in range(1, level):
            l1, l2, r1, r2 = out[prior - 1]
            e0, e1 = END[prior, level, 0], END[prior, level, 1]
            s0, s1 = START[prior, level, 0], START[prior, level, 1]
            p = p + e0[0] * r1 + e1[0] * r2
            t = t + e0[1] * r1 + e1[1] * r2
            s = s + s0[0] * l1 + s1[0] * l2
            u = u + s0[1] * l1 + s1[1] * l2
        l1 = p + ALPHA * s
        r2 = u + BETA * l1
        l2 = l1 + GAMMA * (t + BETA * l1 + r2)
        out.append((l1, l2, s, r2))
    return out


def _boundaries(own_even, own_odd, got_even, got_odd, bnd, count):
    odd = lax.axis_index("row") % 2 == 1

    def read(ref):
        return [ref[pl.ds(k * TILES, count), :] for k in range(6)]

    oe, oo, ge, go = read(own_even), read(own_odd), read(got_even), read(got_odd)

    def pick(yes, no):
        return [jnp.where(odd, y, n) for y, n in zip(yes, no)]

    top = _junction(pick(ge, go), pick(oe, oo))
    low = _junction(pick(oo, oe), pick(go, ge))
    for level in range(3):
        for j in range(4):
            bnd[pl.ds((level * 4 + j) * count, count), :] = (top if j < 2 else low)[level][j]


def _rows_transform(tile, edge):
    row = lax.axis_index("row")
    sub = _sub()
    is7, is0 = sub == 7, sub == 0
    mir7 = is7 & (row == lax.axis_size("row") - 1)
    mir0 = is0 & (row == 0)
    odd = (sub & 1) == 1
    zero = jnp.zeros((8, LANES), F32)

    def up(v, level, j, mirror):
        return jnp.where(mir7, mirror, jnp.where(is7, edge(level, j), pltpu.roll(v, 7, 0)))

    def dn(v, level, j, mirror):
        return jnp.where(mir0, mirror, jnp.where(is0, edge(level, j), pltpu.roll(v, 1, 0)))

    a, b, c, d = tile
    c1 = c + ALPHA * (a + b)
    d1 = d + ALPHA * (b + up(a, 0, 2, b))
    a1 = a + BETA * (dn(d1, 0, 0, c1) + c1)
    b1 = b + BETA * (c1 + d1)
    c2 = c1 + GAMMA * (a1 + b1)
    d2 = d1 + GAMMA * (b1 + up(a1, 0, 3, b1))
    a = (a1 + DELTA * (dn(d2, 0, 1, c2) + c2)) * SCALE_LOW
    b = (b1 + DELTA * (c2 + d2)) * SCALE_LOW
    v = [a, b, c2 * SCALE_HIGH, d2 * SCALE_HIGH]
    b1 = b + ALPHA * (a + up(a, 1, 2, a))
    a1 = a + BETA * (dn(b1, 1, 0, b1) + b1)
    b2 = b1 + GAMMA * (a1 + up(a1, 1, 3, a1))
    x = (a1 + DELTA * (dn(b2, 1, 1, b2) + b2)) * SCALE_LOW
    v += [x, b2 * SCALE_HIGH]
    for ka, kb, j in ((ALPHA, BETA, 0), (GAMMA, DELTA, 1)):
        back = pltpu.roll(x, 1, 0)
        x = x + jnp.where(odd, ka, zero) * (back + up(x, 2, 2 + j, back))
        ahead = pltpu.roll(x, 7, 0)
        x = x + jnp.where(odd, zero, kb) * (dn(x, 2, j, ahead) + ahead)
    v.append(x * jnp.where(odd, SCALE_HIGH, zero + SCALE_LOW))
    return v


def states_kernel(x_ref, even_ref, odd_ref, scr, sems):
    copies = [
        [
            _load(
                x_ref.at[img, rt],
                scr.at[pl.ds(img * CHUNKS, CHUNKS), pl.ds(rt * 8, 8), :],
                sems.at[img, rt],
            )
            for rt in range(4)
        ]
        for img in range(IMAGES)
    ]

    def run(to_end, to_start):
        for img in range(IMAGES):
            for copy in copies[img]:
                copy.wait()
            for c in range(CHUNKS):
                t = tile_row(img, c)
                end, start = _states_of(_rows_of(scr, img * CHUNKS + c))
                for k in range(6):
                    to_end[pl.ds(k * TILES + t, 1), :] = end[k]
                    to_start[pl.ds(k * TILES + t, 1), :] = start[k]

    is_odd = lax.axis_index("row") % 2 == 1
    pl.when(is_odd)(lambda: run(odd_ref, even_ref))
    pl.when(jnp.logical_not(is_odd))(lambda: run(even_ref, odd_ref))


def edges_kernel(x_ref, own_even, own_odd, got_even, got_odd, v_ref, even_ref, odd_ref, bnd):
    _boundaries(own_even, own_odd, got_even, got_odd, bnd, EDGES)
    lane = _lane()
    zero = jnp.zeros((8, LANES), F32)
    tiles = []
    for t in range(EDGES):

        def edge(level, j, t=t):
            return jnp.broadcast_to(bnd[pl.ds((level * 4 + j) * EDGES + t, 1), :], (8, LANES))

        column = (t % IMAGES) * CHUNKS + (t // IMAGES) * (CHUNKS - 1)
        v = _rows_transform(_rows_of(x_ref, column), edge)
        for k in range(7):
            v_ref[t, k] = v[k]
        tiles.append(v)
    is_odd = lax.axis_index("col") % 2 == 1
    for n, (base, count, width) in enumerate(KINDS):
        to_left, to_right = zero, zero
        for img in range(IMAGES):
            for q in range(count):
                slot = (img * count + q) * width
                here = (lane >= slot) & (lane < slot + width)
                start, end = tiles[img][base + q], tiles[IMAGES + img][base + q]
                if slot:
                    start = pltpu.roll(start, slot, 1)
                if (slot + width) % LANES:
                    end = pltpu.roll(end, slot + width, 1)
                to_left = jnp.where(here, start, to_left)
                to_right = jnp.where(here, end, to_right)
        even_ref[pl.ds(8 * n, 8), :] = jnp.where(is_odd, to_left, to_right)
        odd_ref[pl.ds(8 * n, 8), :] = jnp.where(is_odd, to_right, to_left)


def _split(x):
    high = x.astype(jnp.bfloat16)
    return high, (x - high.astype(F32)).astype(jnp.bfloat16)


def _dot(x, w):
    return jnp.dot(x, w, preferred_element_type=F32)


def interior(pairs, later_ref, w_ref, x_ref, own_even, own_odd, got_even, got_odd, edge_ref, scr, lh1, ll1, lh2, ll2, lh3, ll3, bnd, done):
    del later_ref
    _boundaries(own_even, own_odd, got_even, got_odd, bnd, TILES)
    lane = _lane()
    low_half = lane < HALF
    lhs = ((lh1, ll1), (lh2, ll2), (lh3, ll3))

    def build(pair):
        before = None
        for c in range(CHUNKS + 1):
            now = before
            if c < CHUNKS:
                now = []
                for img in pair:

                    def edge(level, j, t=tile_row(img, c)):
                        return jnp.broadcast_to(bnd[pl.ds((level * 4 + j) * TILES + t, 1), :], (8, LANES))

                    v = _rows_transform(_rows_of(x_ref, img * CHUNKS + c), edge)
                    now.append([pltpu.roll(tile, HALF, 1) for tile in v])
            if before is None:
                before = now
            halves = [[jnp.where(low_half, p, q) for p, q in zip(ps, qs)] for ps, qs in zip(before, now)]
            rows1 = [tile for half in halves for tile in half[:4]]
            rows2 = [tile for half in halves for tile in half[4:6]]
            rows3 = [half[6] for half in halves]
            for (high_ref, low_ref), rows in zip(lhs, (rows1, rows2, rows3)):
                high, low = _split(jnp.concatenate(rows, axis=0))
                n = 8 * len(rows)
                for ref, part in ((high_ref, high), (low_ref, low)):
                    if c < CHUNKS:
                        ref[pl.ds(c * n, n), pl.ds(0, LANES)] = part
                    if c:
                        ref[pl.ds((c - 1) * n, n), pl.ds(LANES, LANES)] = part
            before = now

    def multiply(pair):
        outs = []
        for kind, (high_ref, low_ref) in enumerate(lhs):
            both = _dot(high_ref[...], w_ref[kind])
            outs.append(both[:, :LANES] + both[:, LANES:] + _dot(low_ref[...], w_ref[kind, :, :LANES]))
        for c in range(CHUNKS):
            for i, img in enumerate(pair):
                for q in range(4):
                    at = (c * 2 + i) * 32 + q * 8
                    val = outs[0][at : at + 8]
                    if q < 2:
                        at = (c * 2 + i) * 16 + q * 8
                        val = jnp.where((lane & 1) == 0, outs[1][at : at + 8], val)
                    if q < 1:
                        at = (c * 2 + i) * 8
                        val = jnp.where((lane & 3) == 0, outs[2][at : at + 8], val)
                    scr[img * CHUNKS + c, pl.ds(OFFSETS[q], 8, stride=4), :] = val

    for pair in pairs:
        build(pair)
        multiply(pair)
        for img in pair:
            for side, chunk in enumerate((0, CHUNKS - 1)):
                edge_ref[side * IMAGES + img] = scr[img * CHUNKS + chunk]
        done(pair)


def is_early():
    return lax.axis_index("col") % 8 == 0


FIRST, SECOND = (0, 1), (2, 3)


def early_kernel(*refs):
    pl.when(is_early())(lambda: interior((FIRST,), *refs, lambda pair: None))


def late_kernel(*refs):
    ins, (_, kept, out_ref, edge_ref, scr, *rest, sems) = refs[:7], refs[7:]

    def store(pair, source):
        return [
            _load(
                source.at[pl.ds(img * CHUNKS + 1, CHUNKS - 2), pl.ds(rt * 8, 8), :],
                out_ref.at[img, rt, pl.ds(1, CHUNKS - 2)],
                sems.at[img, rt],
            )
            for img in pair
            for rt in range(4)
        ]

    def run(pairs, stores):
        interior(pairs, *ins, edge_ref, scr, *rest, lambda pair: stores.extend(store(pair, scr)))
        for copy in stores:
            copy.wait()

    pl.when(is_early())(lambda: run((SECOND,), store(FIRST, kept)))
    pl.when(jnp.logical_not(is_early()))(lambda: run((FIRST, SECOND), []))


def patch_kernel(w_ref, v_ref, edge_in, got_even, got_odd, dest_ref, out_ref, scr, sems):
    del dest_ref
    col = lax.axis_index("col")
    is_odd = col % 2 == 1
    which = (jnp.where(col == 0, 1, 0), jnp.where(col == lax.axis_size("col") - 1, 2, 0))
    lane = _lane()
    low_half = lane < HALF
    windows = [[[], [], []], [[], [], []]]
    for n, (base, count, width) in enumerate(KINDS):
        via_even, via_odd = got_even[pl.ds(8 * n, 8), :], got_odd[pl.ds(8 * n, 8), :]
        got = (jnp.where(is_odd, via_even, via_odd), jnp.where(is_odd, via_odd, via_even))
        for img in range(IMAGES):
            for q in range(count):
                slot = (img * count + q) * width
                for side, shift in ((0, LANES - slot - width), (1, LANES - slot)):
                    halo = pltpu.roll(got[side], shift % LANES, 1) if shift % LANES else got[side]
                    own = v_ref[side * IMAGES + img, base + q]
                    first, second = (own, halo) if side == 0 else (halo, own)
                    windows[side][n].append(jnp.where(low_half, first, second))
    copies = []
    for side in range(2):
        outs = []
        for n in range(3):
            x = jnp.concatenate(windows[side][n], axis=0)
            y = _dot(jnp.concatenate(_split(x), axis=1), w_ref[which[side], n])
            outs.append(y[:, :LANES] + y[:, LANES:])
        inside = lane < PATCH if side == 0 else lane >= LANES - PATCH
        for img in range(IMAGES):
            t = side * IMAGES + img
            for q in range(4):
                at = (img * 4 + q) * 8
                new = outs[0][at : at + 8]
                if q < 2:
                    at = (img * 2 + q) * 8
                    new = jnp.where((lane & 1) == 0, outs[1][at : at + 8], new)
                if q < 1:
                    new = jnp.where((lane & 3) == 0, outs[2][img * 8 : img * 8 + 8], new)
                where = (t, pl.ds(OFFSETS[q], 8, stride=4), slice(None))
                scr[where] = jnp.where(inside, new, edge_in[where])
            column = scr.reshape(EDGES, 4, 8, LANES).at[t]
            copies.append(_load(column, out_ref.at[img, :, (CHUNKS - 1) * side], sems.at[t]))
    for copy in copies:
        copy.wait()


def pairs(axis):
    n = lax.axis_size(axis)
    even_pairs = [(i, i ^ 1) for i in range(n)]
    odd_pairs = [(i, i + 1 if i % 2 else i - 1) for i in range(1, n - 1)] + [(0, 0), (n - 1, n - 1)]
    return even_pairs, odd_pairs


def swap(axis, even, odd):
    even_pairs, odd_pairs = pairs(axis)
    via_odd = lax.ppermute(odd, axis, odd_pairs)
    via_even = lax.ppermute(even, axis, even_pairs)
    return near(via_even), near(via_odd)


def near(value):
    return pltpu.with_memory_space_constraint(value, pltpu.VMEM)


def held(*dims):
    return pltpu.VMEM(dims, F32)


VMEM = pl.BlockSpec(memory_space=pltpu.VMEM)
ANY = pl.BlockSpec(memory_space=pl.ANY)


def shape(*dims):
    return jax.ShapeDtypeStruct(dims, F32)


def transform(images):
    x = images.reshape(IMAGES, 4, 8, CHUNKS, LANES).transpose(0, 1, 3, 2, 4)
    dma = pltpu.SemaphoreType.DMA
    row_even, row_odd, block = pl.pallas_call(
        states_kernel,
        out_shape=(held(6 * TILES, LANES), held(6 * TILES, LANES), held(TILES, ROWS, LANES)),
        in_specs=[ANY],
        out_specs=(VMEM,) * 3,
        scratch_shapes=[dma((IMAGES, 4))],
        compiler_params=pltpu.CompilerParams(vmem_limit_bytes=8 << 20),
        name="row_states",
    )(pltpu.with_memory_space_constraint(x, pltpu.HBM))
    got_even, got_odd = swap("row", row_even, row_odd)
    rows = (near(block), near(row_even), near(row_odd), got_even, got_odd)
    v_edge, col_even, col_odd = pl.pallas_call(
        edges_kernel,
        out_shape=(held(EDGES, 7, 8, LANES), held(24, LANES), held(24, LANES)),
        in_specs=[VMEM] * 5,
        out_specs=(VMEM,) * 3,
        scratch_shapes=[pltpu.VMEM((12 * EDGES, LANES), F32)],
        compiler_params=pltpu.CompilerParams(vmem_limit_bytes=8 << 20),
        name="edge_rows",
    )(*rows)
    edge_matrices = near(jnp.asarray(EDGE))
    operands = (edge_matrices, near(jnp.asarray(LINE)), *rows)
    work = [
        *(pltpu.VMEM((CHUNKS * n, 2 * LANES), jnp.bfloat16) for n in (64, 64, 32, 32, 16, 16)),
        pltpu.VMEM((12 * TILES, LANES), F32),
    ]
    settings = dict(
        cost_estimate=pl.CostEstimate(flops=40_000_000, transcendentals=0, bytes_accessed=2_000_000),
        compiler_params=pltpu.CompilerParams(vmem_limit_bytes=24 << 20),
    )
    even_pairs, odd_pairs = pairs("col")
    halo_even = lax.ppermute(col_even, "col", even_pairs)
    out_edge, kept = pl.pallas_call(
        early_kernel,
        out_shape=(held(EDGES, ROWS, LANES), held(TILES, ROWS, LANES)),
        in_specs=[VMEM] * 7,
        out_specs=(VMEM, VMEM),
        scratch_shapes=work,
        name="interior_early",
        **settings,
    )(*operands)
    col_odd, out_edge = lax.optimization_barrier((col_odd, out_edge))
    halo_odd = lax.ppermute(near(col_odd), "col", odd_pairs)
    out, out_edge = pl.pallas_call(
        late_kernel,
        out_shape=(shape(IMAGES, 4, CHUNKS, 8, LANES), held(EDGES, ROWS, LANES)),
        in_specs=[VMEM] * 9,
        out_specs=(ANY, VMEM),
        input_output_aliases={7: 1},
        scratch_shapes=[pltpu.VMEM((TILES, ROWS, LANES), F32), *work, dma((IMAGES, 4))],
        name="interior_late",
        **settings,
    )(*operands, near(out_edge), near(kept))
    halo_even, halo_odd = near(halo_even), near(halo_odd)
    out = pl.pallas_call(
        patch_kernel,
        out_shape=shape(IMAGES, 4, CHUNKS, 8, LANES),
        in_specs=[VMEM] * 5 + [ANY],
        out_specs=ANY,
        input_output_aliases={5: 0},
        scratch_shapes=[pltpu.VMEM((EDGES, ROWS, LANES), F32), dma((EDGES,))],
        compiler_params=pltpu.CompilerParams(vmem_limit_bytes=8 << 20),
        name="edge_columns",
    )(edge_matrices, near(v_edge), near(out_edge), halo_even, halo_odd, out)
    return out.transpose(0, 1, 3, 2, 4).reshape(IMAGES, ROWS, CHUNKS * LANES)


def solution(mesh):
    return jax.shard_map(
        transform,
        mesh=mesh,
        in_specs=(P(None, "row", "col"),),
        out_specs=P(None, "row", "col"),
        check_vma=False,
    )
```
